128 devices in a mesh: seq: 4 (over x), head: 32 (over y, z, core).
Axes of the slice: x: 4, y: 4, z: 4, core: 2. Of those that a mesh axis runs over, the one named last changes fastest.
Arguments:
- queries: bfloat16 [32768, 4096], P(('seq', 'head')), may hold values from -6 to 6
- key_vectors: bfloat16 [32768, 4096], P(('seq', 'head')), may hold values from -0.375 to 0.375
- values: bfloat16 [32768, 8192], P(('seq', 'head')), may hold values from -6 to 6
- decay_log: bfloat16 [32768, 16], P(('seq', 'head')), may hold values from -0.8 to 0, as said below
- gate_input: bfloat16 [32768, 8192], P(('seq', 'head')), may hold values from -6 to 6
Outputs:
- retention_out: bfloat16 [32768, 8192], P(('seq', 'head'))
The draws below stay inside these ranges and needn't reach their ends.
Inputs may be any that keep to these rules, and one draw needn't show every extreme that they name: `decay_log`: every entry is negative.
All inputs are finite; a program needn't handle non-finite values.
Results may differ from the reference program's by a relative error of at most 0.0063.
Values may be sent and summed in bfloat16 or wider, within the bound.
No kernel may reach another device: no remote copies, remote signals or barrier semaphores. Data moves between devices by JAX's collectives and lax.ppermute only.
A program may use at most 128 MiB of HBM per device.

```python
import math
import jax
import jax.numpy as jnp
from jax import lax

RETAIN_HEADS = 16
DK = 256
DV = 512
BLOCK = 512
DOC_POSITIONS = 32768


def draw_decay_log(key, part):
    key_kind, key_slow, key_fast, key_rough, key_location, key_magnitude, key_medium = jax.random.split(key, 7)
    fast_count = 4
    medium_count = 4
    medium_low = math.log(1.0 / 600.0)
    medium_high = math.log(1.0 / 300.0)
    head_rank = jax.random.permutation(key_kind, jnp.arange(RETAIN_HEADS, dtype=jnp.int32))
    fast_heads = head_rank < fast_count
    medium_heads = jnp.logical_and(head_rank >= fast_count, head_rank < fast_count + medium_count)
    slow_rate = jnp.exp(jax.random.uniform(key_slow, (RETAIN_HEADS,), jnp.float32, math.log(0.2), math.log(0.5))) / DOC_POSITIONS
    fast_rate = jnp.exp(jax.random.uniform(key_fast, (RETAIN_HEADS,), jnp.float32, math.log(1.0 / 50.0), math.log(1.0 / 30.0)))
    medium_rate = jnp.exp(jax.random.uniform(key_medium, (RETAIN_HEADS,), jnp.float32, medium_low, medium_high))
    head_decay_rate = jnp.where(fast_heads, fast_rate, jnp.where(medium_heads, medium_rate, slow_rate))
    jaggedness = jnp.exp(jax.random.uniform(key_rough, (DOC_POSITIONS, RETAIN_HEADS), jnp.float32, math.log(0.5), math.log(2.0)))
    key_first, key_gap = jax.random.split(key_location)
    first_spot = jax.random.randint(key_first, (RETAIN_HEADS,), 0, DOC_POSITIONS)
    spot_gap = jax.random.randint(key_gap, (RETAIN_HEADS,), 0, DOC_POSITIONS - 1)
    second_spot = (first_spot + 1 + spot_gap) % DOC_POSITIONS
    spike_magnitude = jax.random.uniform(key_magnitude, (2, RETAIN_HEADS), jnp.float32, math.log(0.5), math.log(0.8))
    token_offset = jnp.arange(DOC_POSITIONS)[:, None]
    decay_spikes = jnp.where(token_offset == first_spot[None, :], spike_magnitude[0][None, :], 0.0)
    decay_spikes = decay_spikes + jnp.where(token_offset == second_spot[None, :], spike_magnitude[1][None, :], 0.0)
    return (decay_spikes - head_decay_rate[None, :] * jaggedness).astype(jnp.bfloat16)


def block_scale(key, extent, cuts, low, high):
    level, own = 1.0, jax.random.fold_in(key, 6)
    for dim, shards_of in cuts:
        heights = jnp.exp(jax.random.uniform(jax.random.fold_in(own, dim), (shards_of,), jnp.float32, low / len(cuts), high / len(cuts)))
        level = level * jnp.repeat(heights, extent[dim] // shards_of).reshape([-1 if axis == dim else 1 for axis in range(len(extent))])
    return level


def bell_draw(own_key, shape, deviation, reach, shards=(), held_as=jnp.bfloat16):
    factor_of = block_scale(own_key, shape, shards, -0.22, 0.18) if shards else 1.0
    array = jax.random.normal(own_key, shape, jnp.float32) * deviation * factor_of
    return jnp.minimum(jnp.maximum(array, -reach), reach).astype(held_as)


def setup_inputs(seed: int = 0) -> dict:
    key_of = jax.random.split(jax.random.key(seed), 6)
    return {
        "queries": bell_draw(key_of[0], (DOC_POSITIONS, RETAIN_HEADS * DK), 1.0, 6.0, ((0, 128),)),
        "key_vectors": bell_draw(key_of[1], (DOC_POSITIONS, RETAIN_HEADS * DK), 0.0625, 0.375, ((0, 128),)),
        "values": bell_draw(key_of[2], (DOC_POSITIONS, RETAIN_HEADS * DV), 1.0, 6.0, ((0, 128),)),
        "decay_log": draw_decay_log(jax.random.fold_in(key_of[5], 71), 0),
        "gate_input": bell_draw(key_of[4], (DOC_POSITIONS, RETAIN_HEADS * DV), 1.0, 6.0, ((0, 128),)),
    }


def reference(queries, key_vectors, values, decay_log, gate_input):
    blocks = DOC_POSITIONS // BLOCK
    query_blocks = queries.reshape(blocks, BLOCK, RETAIN_HEADS, DK)
    key_blocks = key_vectors.reshape(blocks, BLOCK, RETAIN_HEADS, DK)
    value_blocks = values.reshape(blocks, BLOCK, RETAIN_HEADS, DV)
    decay_blocks = decay_log.astype(jnp.float32).reshape(blocks, BLOCK, RETAIN_HEADS)
    causal = jnp.arange(BLOCK)[:, None] >= jnp.arange(BLOCK)[None, :]

    def advance(carried_state, pieces):
        query_block, key_block, value_block, decay_block = pieces
        running = jnp.cumsum(decay_block, axis=0)
        block_decay = running[-1]
        faded = (key_block.astype(jnp.float32) * jnp.exp(block_decay[None, :] - running)[:, :, None]).astype(jnp.bfloat16)
        state_low = carried_state.astype(jnp.bfloat16)
        spread = running.T[:, :, None] - running.T[:, None, :]
        factor = jnp.exp(jnp.where(causal[None], spread, -jnp.inf))
        scores = jnp.einsum('ihd,jhd->hij', query_block.astype(jnp.float32), key_block.astype(jnp.float32))
        weights = (scores * factor).astype(jnp.bfloat16)
        within = jnp.einsum('hij,jhw->ihw', weights.astype(jnp.float32), value_block.astype(jnp.float32))
        across = jnp.einsum('ihd,hdw->ihw', query_block.astype(jnp.float32), state_low.astype(jnp.float32))
        across = across * jnp.exp(running)[:, :, None]
        retained = (within + across).astype(jnp.bfloat16)
        additions = jnp.einsum('jhd,jhw->hdw', faded.astype(jnp.float32), value_block.astype(jnp.float32))
        updated = jnp.exp(block_decay)[:, None, None] * carried_state + additions
        return (updated, retained)
    initial = jnp.zeros((RETAIN_HEADS, DK, DV), jnp.float32)
    unused, retained = lax.scan(advance, initial, (query_blocks, key_blocks, value_blocks, decay_blocks))
    retained = retained.reshape(DOC_POSITIONS, RETAIN_HEADS, DV).astype(jnp.float32)
    average = lax.optimization_barrier(jnp.mean(retained, axis=2, keepdims=True))
    centered = retained - average
    variance = lax.optimization_barrier(jnp.mean(centered * centered, axis=2, keepdims=True))
    normed = centered / jnp.sqrt(variance + 1e-06)
    gated = jax.nn.silu(gate_input.astype(jnp.float32).reshape(DOC_POSITIONS, RETAIN_HEADS, DV)) * normed
    return gated.astype(jnp.bfloat16).reshape(DOC_POSITIONS, RETAIN_HEADS * DV)
```

```python
import functools

import jax
import jax.numpy as jnp
from jax import lax
from jax.experimental import pallas as pl
from jax.experimental.pallas import tpu as pltpu
from jax.sharding import Mesh, PartitionSpec as P

HEADS = 16
DK = 256
DV = 512
ROWS = 256
HALF = HEADS // 2
CHIPS = 64
SLICES = CHIPS // HALF
PIECE = DK // SLICES
TILES = DV // 128
SLICE = PIECE * TILES
SENT = SLICE + 8

f32 = jnp.float32
bf16 = jnp.bfloat16


def triangle():
    rows = lax.broadcasted_iota(jnp.int32, (ROWS, ROWS), 0)
    cols = lax.broadcasted_iota(jnp.int32, (ROWS, ROWS), 1)
    return rows >= cols


def running_of(decay):
    return jnp.dot(triangle().astype(f32).astype(bf16), decay, preferred_element_type=f32)


def running_rows(decay):
    ones = triangle().astype(f32).astype(bf16)
    return lax.dot_general(decay, ones, (((0,), (1,)), ((), ())), preferred_element_type=f32)


def column(table, head):
    lanes = lax.broadcasted_iota(jnp.int32, table.shape, 1)
    return jnp.sum(jnp.where(lanes == head, table, 0.0), axis=1, keepdims=True)


def chunk_state(key, value, run, head):
    fade = column(jnp.exp(run[ROWS - 1 : ROWS, :] - run), head)
    faded = (key.astype(f32) * fade).astype(bf16)
    return lax.dot_general(faded, value, (((0,), (0,)), ((), ())), preferred_element_type=f32)


def put_slices(ref, state):
    for o in range(SLICES):
        for t in range(TILES):
            ref[o, t * PIECE : (t + 1) * PIECE, :] = state[
                o * PIECE : (o + 1) * PIECE, t * 128 : (t + 1) * 128
            ]


def get_slices(ref):
    cols = [
        ref[:, t * PIECE : (t + 1) * PIECE, :].reshape(DK, 128) for t in range(TILES)
    ]
    return jnp.concatenate(cols, axis=1)


def partner_state_kernel(core_ref, key_ref, value_ref, decay_ref, out_ref, run_ref):
    step = pl.program_id(0)

    @pl.when(step == 0)
    def _():
        run_ref[...] = running_of(decay_ref[...])

    head = (1 - core_ref[0]) * HALF + step
    state = chunk_state(key_ref[...], value_ref[...], run_ref[...], head)
    put_slices(out_ref, state.astype(bf16))


def own_state_kernel(
    core_ref, key_ref, value_ref, decay_ref, other_ref, got_ref,
    out_ref, first_ref, damp_ref, run_ref, other_run_ref,
):
    step = pl.program_id(0)

    @pl.when(step == 0)
    def _():
        run_ref[...] = running_of(decay_ref[...])
        other_run_ref[...] = running_of(other_ref[...])

    core = core_ref[0]
    head = core * HALF + step
    run = run_ref[...]
    own = chunk_state(key_ref[...], value_ref[...], run, head)
    got = get_slices(got_ref).astype(f32)
    total = column(run[ROWS - 8 :, :], head)[7:8, :]
    other_total = column(other_run_ref[ROWS - 8 :, :], head)[7:8, :]
    is_first = core == 0
    own_rate = jnp.exp(jnp.where(is_first, other_total, 0.0))
    got_rate = jnp.exp(jnp.where(is_first, 0.0, total))
    both = own * own_rate + got * got_rate
    put_slices(out_ref, both.astype(bf16))
    put_slices(first_ref, jnp.where(is_first, own, got).astype(bf16))
    damping = jnp.broadcast_to(jnp.exp(total + other_total), (8, 128))
    high = damping.astype(bf16).astype(f32)
    rest = damping - high
    middle = rest.astype(bf16).astype(f32)
    low = rest - middle
    rows = lax.broadcasted_iota(jnp.int32, (8, 128), 0)
    parts = jnp.where(rows == 0, high, jnp.where(rows == 1, middle, low)).astype(bf16)
    for o in range(SLICES):
        out_ref[o, SLICE:SENT, :] = parts
    first_total = jnp.where(is_first, total, other_total)
    damp_ref[0] = jnp.broadcast_to(jnp.exp(first_total), (8, 128))


def within_kernel(query_ref, key_ref, value_ref, decay_ref, out_ref, run_ref, rows_ref):
    head = pl.program_id(0)

    @pl.when(head == 0)
    def _():
        run_ref[...] = running_of(decay_ref[...])
        rows_ref[...] = running_rows(decay_ref[...])

    scores = lax.dot_general(
        query_ref[...], key_ref[...], (((1,), (1,)), ((), ())), preferred_element_type=f32
    )
    spread = column(run_ref[...], head) - rows_ref[pl.ds(head, 1), :]
    factor = jnp.exp(jnp.where(triangle(), spread, -jnp.inf))
    weights = (scores * factor).astype(bf16)
    out_ref[...] = jnp.dot(weights, value_ref[...], preferred_element_type=f32)


STEP = 8


def prefix_kernel(in_ref, out_ref, state_ref):
    @pl.when(pl.program_id(0) == 0)
    def _():
        state_ref[...] = jnp.zeros_like(state_ref)

    state = state_ref[...]
    for b in range(STEP):
        parts = in_ref[b, SLICE:SENT, :].astype(f32)
        damping = parts[0:1] + parts[1:2] + parts[2:3]
        out_ref[b] = state.astype(bf16)
        state = damping * state + in_ref[b, :SLICE, :].astype(f32)
    state_ref[...] = state


def middle_kernel(core_ref, start_ref, first_ref, damp_ref, send_ref, use_ref):
    is_first = core_ref[0] == 0
    start = start_ref[...].astype(f32)
    middle = start * damp_ref[0, 0:1, :][None] + first_ref[...].astype(f32)
    send_ref[...] = jnp.where(is_first, middle, start).astype(bf16)
    use_ref[...] = jnp.where(is_first, start, middle).astype(bf16)


def finish_kernel(group_ref, query_ref, start_ref, within_ref, gate_ref, decay_ref, *rest):
    out_ref, run_ref = rest[-2:]
    step = pl.program_id(0)

    @pl.when(step == 0)
    def _():
        run_ref[...] = running_of(decay_ref[...])

    head = group_ref[0] * HALF + step
    across = jnp.dot(query_ref[...], get_slices(start_ref), preferred_element_type=f32)
    retained = within_ref[...] + across * jnp.exp(column(run_ref[...], head))
    average = jnp.mean(retained, axis=1, keepdims=True)
    centered = retained - average
    variance = jnp.mean(centered * centered, axis=1, keepdims=True)
    normed = centered * lax.rsqrt(variance + 1e-06)
    gate = gate_ref[...].astype(f32)
    out_ref[...] = (gate / (1.0 + jnp.exp(-gate)) * normed).astype(bf16)


def call(kernel, name, grid, in_specs, out_specs, out_shape, scratch, flops, aliases=None):
    return pl.pallas_call(
        kernel,
        out_shape=out_shape,
        grid_spec=pltpu.PrefetchScalarGridSpec(
            num_scalar_prefetch=1,
            grid=(grid,),
            in_specs=in_specs,
            out_specs=out_specs,
            scratch_shapes=scratch,
        ),
        compiler_params=pltpu.CompilerParams(dimension_semantics=("arbitrary",)),
        cost_estimate=pl.CostEstimate(flops=flops, transcendentals=0, bytes_accessed=0),
        input_output_aliases=aliases or {},
        name=name,
    )


def shape(*dims, dtype=bf16):
    return jax.ShapeDtypeStruct(dims, dtype)


def shards(queries, key_vectors, values, decay_log, gate_input):
    core = lax.axis_index("core").astype(jnp.int32).reshape(1)
    swap = [(0, 1), (1, 0)]
    other_decay = lax.ppermute(decay_log, "core", swap)

    whole = pl.BlockSpec((ROWS, HEADS), lambda i, c: (0, 0))
    own = lambda width: pl.BlockSpec((ROWS, width), lambda i, c: (0, c[0] * HALF + i))
    theirs = lambda width: pl.BlockSpec((ROWS, width), lambda i, c: (0, (1 - c[0]) * HALF + i))
    slices = pl.BlockSpec((SLICES, SLICE, 128), lambda i, c: (i, 0, 0))
    sent = pl.BlockSpec((SLICES, SENT, 128), lambda i, c: (i, 0, 0))
    damp = pl.BlockSpec((1, 8, 128), lambda i, c: (i, 0, 0))
    table = pltpu.VMEM((ROWS, HEADS), f32)

    theirs_state = call(
        partner_state_kernel, "partner_state", HALF, [theirs(DK), theirs(DV), whole], slices,
        shape(CHIPS, SLICE, 128), [table], 2 * HALF * ROWS * DK * DV,
    )(core, key_vectors, values, decay_log)
    got = lax.ppermute(theirs_state, "core", swap)
    block_state, first_state, damping = call(
        own_state_kernel, "own_state", HALF,
        [own(DK), own(DV), whole, whole, slices], [sent, slices, damp],
        [shape(CHIPS, SENT, 128), shape(CHIPS, SLICE, 128), shape(HALF, 8, 128, dtype=f32)],
        [table, table], 2 * HALF * ROWS * DK * DV,
    )(core, key_vectors, values, decay_log, other_decay, got)
    everyone = ("seq", "chip")
    collected = lax.all_to_all(block_state, everyone, 0, 0, tiled=True)

    head_block = lambda width: pl.BlockSpec((ROWS, width), lambda i: (0, i))
    within = pl.pallas_call(
        within_kernel,
        out_shape=shape(ROWS, HEADS * DV, dtype=f32),
        grid=(HEADS,),
        in_specs=[head_block(DK), head_block(DK), head_block(DV), pl.BlockSpec((ROWS, HEADS), lambda i: (0, 0))],
        out_specs=head_block(DV),
        scratch_shapes=[table, pltpu.VMEM((HEADS, ROWS), f32)],
        compiler_params=pltpu.CompilerParams(dimension_semantics=("arbitrary",)),
        cost_estimate=pl.CostEstimate(flops=2 * HEADS * ROWS * ROWS * (DK + DV), transcendentals=0, bytes_accessed=0),
        name="within",
    )(queries, key_vectors, values, decay_log)

    starts = pl.pallas_call(
        prefix_kernel,
        out_shape=shape(CHIPS, SLICE, 128),
        grid=(CHIPS // STEP,),
        in_specs=[pl.BlockSpec((STEP, SENT, 128), lambda i: (i, 0, 0))],
        out_specs=pl.BlockSpec((STEP, SLICE, 128), lambda i: (i, 0, 0)),
        scratch_shapes=[pltpu.VMEM((SLICE, 128), f32)],
        compiler_params=pltpu.CompilerParams(dimension_semantics=("arbitrary",)),
        name="prefix",
    )(collected)
    start = lax.all_to_all(starts, everyone, 0, 0, tiled=True)
    send, use = call(
        middle_kernel, "middle", HALF, [slices, slices, damp], [slices, slices],
        [shape(CHIPS, SLICE, 128)] * 2, [], 4 * CHIPS * SLICE * 128,
    )(core, start, first_state, damping)
    their_use = lax.ppermute(send, "core", swap)

    specs = [own(DK), slices, own(DV), own(DV), whole]
    flops = 2 * HALF * ROWS * DK * DV
    half = call(
        finish_kernel, "finish_own", HALF, specs, own(DV), shape(ROWS, HEADS * DV), [table], flops,
    )(core, queries, use, within, gate_input, decay_log)
    return call(
        finish_kernel, "finish_theirs", HALF, specs + [pl.BlockSpec(memory_space=pl.ANY)], own(DV),
        shape(ROWS, HEADS * DV), [table], flops, {6: 0},
    )(1 - core, queries, their_use, within, gate_input, decay_log, half)


def solution(mesh):
    mesh = Mesh(mesh.devices.reshape(4, 16, 2), ("seq", "chip", "core"))
    spec = P(("seq", "chip", "core"), None)
    return jax.shard_map(
        shards, mesh=mesh, in_specs=(spec,) * 5, out_specs=spec, check_vma=False
    )
```

```python
import jax
import jax.numpy as jnp
from jax import lax
from jax.experimental import pallas as pl
from jax.experimental.pallas import tpu as pltpu
from jax.sharding import Mesh, PartitionSpec as P

HEADS = 16
DK = 256
DV = 512
ROWS = 256
HALF = HEADS // 2
CHIPS = 64
SLICES = CHIPS // HALF
PIECE = DK // SLICES
TILES = DV // 128
SLICE = PIECE * TILES
SENT = SLICE + 8
PER_STEP = 4
BLOCKS_PER_STEP = 32

f32 = jnp.float32
bf16 = jnp.bfloat16


def triangle():
    rows = lax.broadcasted_iota(jnp.int32, (ROWS, ROWS), 0)
    cols = lax.broadcasted_iota(jnp.int32, (ROWS, ROWS), 1)
    return rows >= cols


def running_of(decay):
    ones = triangle().astype(f32).astype(bf16)
    return lax.dot_general(ones, decay, (((1,), (1,)), ((), ())), preferred_element_type=f32)


def running_rows(decay):
    ones = triangle().astype(f32).astype(bf16)
    return lax.dot_general(decay, ones, (((1,), (1,)), ((), ())), preferred_element_type=f32)


def column(table, head):
    lanes = lax.broadcasted_iota(jnp.int32, table.shape, 1)
    return jnp.sum(jnp.where(lanes == head, table, 0.0), axis=1, keepdims=True)


def put_slices(ref, at, state):
    for o in range(SLICES):
        for t in range(TILES):
            ref[at * SLICES + o, t * PIECE : (t + 1) * PIECE, :] = state[
                o * PIECE : (o + 1) * PIECE, t * 128 : (t + 1) * 128
            ]


def get_slices(ref, at):
    cols = [
        ref[at * SLICES : (at + 1) * SLICES, t * PIECE : (t + 1) * PIECE, :].reshape(DK, 128)
        for t in range(TILES)
    ]
    return jnp.concatenate(cols, axis=1)


def state_kernel(group_ref, key_ref, value_ref, decay_ref, out_ref, fade_ref):
    step = pl.program_id(0)

    @pl.when(step == 0)
    def _():
        run = running_of(decay_ref[...])
        fade_ref[...] = jnp.exp(run[ROWS - 1 : ROWS, :] - run)

    for n in range(PER_STEP):
        fade = column(fade_ref[...], group_ref[0] * HALF + step * PER_STEP + n)
        faded = (key_ref[:, n * DK : (n + 1) * DK].astype(f32) * fade).astype(bf16)
        state = lax.dot_general(
            faded, value_ref[:, n * DV : (n + 1) * DV], (((0,), (0,)), ((), ())),
            preferred_element_type=f32,
        )
        put_slices(out_ref, n, state.astype(bf16))


def combine_kernel(core_ref, own_ref, got_ref, decay_ref, other_ref, out_ref, rate_ref):
    step = pl.program_id(0)
    is_first = core_ref[0] == 0

    @pl.when(step == 0)
    def _():
        ones = jnp.ones((128, ROWS), f32).astype(bf16)
        total = lax.dot_general(
            decay_ref[...], ones, (((1,), (1,)), ((), ())), preferred_element_type=f32
        )
        other = lax.dot_general(
            other_ref[...], ones, (((1,), (1,)), ((), ())), preferred_element_type=f32
        )
        rate_ref[0] = jnp.exp(jnp.where(is_first, other, 0.0))
        rate_ref[1] = jnp.exp(jnp.where(is_first, 0.0, total))
        rate_ref[2] = jnp.exp(total + other)

    rows = lax.broadcasted_iota(jnp.int32, (8, 128), 0)
    for n in range(PER_STEP):
        head = pl.ds(core_ref[0] * HALF + step * PER_STEP + n, 1)
        own_rate = rate_ref[0, head, :]
        got_rate = rate_ref[1, head, :]
        damping = rate_ref[2, head, :]
        high = damping.astype(bf16).astype(f32)
        rest = damping - high
        middle = rest.astype(bf16).astype(f32)
        parts = jnp.where(rows == 0, high, jnp.where(rows == 1, middle, rest - middle))
        parts = parts.astype(bf16)
        for o in range(n * SLICES, (n + 1) * SLICES):
            both = own_ref[o].astype(f32) * own_rate + got_ref[o].astype(f32) * got_rate
            out_ref[o, :SLICE, :] = both.astype(bf16)
            out_ref[o, SLICE:SENT, :] = parts


def within_kernel(
    core_ref, *refs,
):
    own, theirs = refs[0:4], refs[4:8]
    decay_ref, other_ref, own_out, theirs_out, reach_out, run_ref, rows_ref, reach_ref = refs[8:]
    step = pl.program_id(0)
    core = core_ref[0]

    @pl.when(step == 0)
    def _():
        run = running_of(decay_ref[...])
        run_ref[...] = run
        rows_ref[...] = running_rows(decay_ref[...])
        other = running_of(other_ref[...])[ROWS - 1 : ROWS, :]
        reach_out[...] = jnp.exp(run + jnp.where(core == 0, 0.0, other))
        reach_ref[...] = jnp.where(core == 0, 0.0, jnp.exp(run))

    for group, ins, out_ref in ((core, own, own_out), (1 - core, theirs, theirs_out)):
        query_ref, key_ref, value_ref, state_ref = ins
        head = group * HALF + step
        query = query_ref[...]
        scores = lax.dot_general(
            query, key_ref[...], (((1,), (1,)), ((), ())), preferred_element_type=f32
        )
        spread = column(run_ref[...], head) - rows_ref[pl.ds(head, 1), :]
        factor = jnp.exp(jnp.where(triangle(), spread, -jnp.inf))
        weights = (scores * factor).astype(bf16)
        local = jnp.dot(weights, value_ref[...], preferred_element_type=f32)
        before = jnp.dot(query, get_slices(state_ref, 0), preferred_element_type=f32)
        out_ref[...] = local + before * column(reach_ref[...], head)


def prefix_kernel(in_ref, out_ref, state_ref):
    @pl.when(pl.program_id(0) == 0)
    def _():
        state_ref[...] = jnp.zeros_like(state_ref)

    state = state_ref[...]
    for b in range(BLOCKS_PER_STEP):
        parts = in_ref[b, SLICE:SENT, :].astype(f32)
        damping = parts[0:1] + parts[1:2] + parts[2:3]
        out_ref[b] = state.astype(bf16)
        state = damping * state + in_ref[b, :SLICE, :].astype(f32)
    state_ref[...] = state


def finish_kernel(group_ref, query_ref, start_ref, within_ref, gate_ref, reach_ref, *rest):
    out_ref = rest[-1]
    for n in range(PER_STEP):
        head = group_ref[0] * HALF + pl.program_id(0) * PER_STEP + n
        wide = slice(n * DV, (n + 1) * DV)
        across = jnp.dot(
            query_ref[:, n * DK : (n + 1) * DK], get_slices(start_ref, n),
            preferred_element_type=f32,
        )
        retained = within_ref[:, wide] + across * column(reach_ref[...], head)
        average = jnp.mean(retained, axis=1, keepdims=True)
        centered = retained - average
        variance = jnp.mean(centered * centered, axis=1, keepdims=True)
        normed = centered * lax.rsqrt(variance + 1e-06)
        gate = gate_ref[:, wide].astype(f32)
        out_ref[:, wide] = (gate / (1.0 + jnp.exp(-gate)) * normed).astype(bf16)


def call(kernel, name, grid, in_specs, out_specs, out_shape, scratch, flops, aliases=None):
    return pl.pallas_call(
        kernel,
        out_shape=out_shape,
        grid_spec=pltpu.PrefetchScalarGridSpec(
            num_scalar_prefetch=1,
            grid=(grid,),
            in_specs=in_specs,
            out_specs=out_specs,
            scratch_shapes=scratch,
        ),
        compiler_params=pltpu.CompilerParams(dimension_semantics=("arbitrary",)),
        cost_estimate=pl.CostEstimate(flops=flops, transcendentals=0, bytes_accessed=0),
        input_output_aliases=aliases or {},
        name=name,
    )


def shape(*dims, dtype=bf16):
    return jax.ShapeDtypeStruct(dims, dtype)


def shards(queries, key_vectors, values, decay_log, gate_input):
    core = lax.axis_index("core").astype(jnp.int32).reshape(1)
    other = 1 - core
    swap = [(0, 1), (1, 0)]
    everyone = ("seq", "chip")
    decay = decay_log.T
    other_decay = lax.ppermute(decay, "core", swap)

    steps = HALF // PER_STEP
    whole = lambda *dims: pl.BlockSpec(dims, lambda i, c: (0,) * len(dims))
    heads = lambda width, n=PER_STEP: pl.BlockSpec(
        (ROWS, width * n), lambda i, c: (0, c[0] * (HALF // n) + i)
    )
    theirs = lambda width: pl.BlockSpec((ROWS, width), lambda i, c: (0, (1 - c[0]) * HALF + i))
    half = lambda width, n=PER_STEP: pl.BlockSpec((ROWS, width * n), lambda i, c: (0, i))
    pieces = lambda n=PER_STEP: pl.BlockSpec((SLICES * n, SLICE, 128), lambda i, c: (i, 0, 0))
    sent = pl.BlockSpec((SLICES * PER_STEP, SENT, 128), lambda i, c: (i, 0, 0))
    decays = whole(HEADS, ROWS)
    table = pltpu.VMEM((ROWS, HEADS), f32)
    flops = 2 * HALF * ROWS * DK * DV

    def chunk_states(group, name):
        return call(
            state_kernel, name, steps, [heads(DK), heads(DV), decays], pieces(),
            shape(CHIPS, SLICE, 128), [table], flops,
        )(group, key_vectors, values, decay)

    theirs_state = chunk_states(other, "theirs_state")
    got = lax.ppermute(theirs_state, "core", swap)
    own_state = chunk_states(core, "own_state")
    block_state = call(
        combine_kernel, "combine", steps, [pieces(), pieces(), decays, decays], sent,
        shape(CHIPS, SENT, 128), [pltpu.VMEM((3, HEADS, 128), f32)], flops // 8,
    )(core, own_state, got, decay, other_decay)
    block_state, late_decay, late_state = lax.optimization_barrier((block_state, decay, own_state))
    collected = lax.all_to_all(block_state, everyone, 0, 0, tiled=True)
    their_first = lax.ppermute(late_state, "core", swap)

    own_within, their_within, reach = call(
        within_kernel, "within", HALF,
        [heads(DK, 1), heads(DK, 1), heads(DV, 1), pieces(1),
         theirs(DK), theirs(DK), theirs(DV), pieces(1), decays, decays],
        [half(DV, 1), half(DV, 1), whole(ROWS, HEADS)],
        [shape(ROWS, HALF * DV, dtype=f32)] * 2 + [shape(ROWS, HEADS, dtype=f32)],
        [table, pltpu.VMEM((HEADS, ROWS), f32), table], 4 * flops,
    )(core, queries, key_vectors, values, got, queries, key_vectors, values, their_first,
      late_decay, other_decay)
    collected, own_within = lax.optimization_barrier((collected, own_within))

    starts = pl.pallas_call(
        prefix_kernel,
        out_shape=shape(CHIPS, SLICE, 128),
        grid=(CHIPS // BLOCKS_PER_STEP,),
        in_specs=[pl.BlockSpec((BLOCKS_PER_STEP, SENT, 128), lambda i: (i, 0, 0))],
        out_specs=pl.BlockSpec((BLOCKS_PER_STEP, SLICE, 128), lambda i: (i, 0, 0)),
        scratch_shapes=[pltpu.VMEM((SLICE, 128), f32)],
        compiler_params=pltpu.CompilerParams(dimension_semantics=("arbitrary",)),
        name="prefix",
    )(collected)
    start = lax.all_to_all(starts, everyone, 0, 0, tiled=True)
    their_start = lax.ppermute(start, "core", swap)

    specs = [heads(DK), pieces(), half(DV), heads(DV), whole(ROWS, HEADS)]
    result = shape(ROWS, HEADS * DV)
    done = call(finish_kernel, "finish_own", steps, specs, heads(DV), result, [], flops)(
        core, queries, start, own_within, gate_input, reach
    )
    return call(
        finish_kernel, "finish_theirs", steps, specs + [pl.BlockSpec(memory_space=pl.ANY)],
        heads(DV), result, [], flops, {6: 0},
    )(other, queries, their_start, their_within, gate_input, reach, done)


def solution(mesh):
    mesh = Mesh(mesh.devices.reshape(4, 16, 2), ("seq", "chip", "core"))
    spec = P(("seq", "chip", "core"), None)
    return jax.shard_map(
        shards, mesh=mesh, in_specs=(spec,) * 5, out_specs=spec, check_vma=False
    )
```

```python
import jax
import jax.numpy as jnp
from jax import lax
from jax.experimental import pallas as pl
from jax.experimental.pallas import tpu as pltpu
from jax.sharding import Mesh, PartitionSpec as P

HEADS = 16
DK = 256
DV = 512
ROWS = 256
HALF = HEADS // 2
LINE = 4
GROUPS = 2
GROUP = HALF // GROUPS
PIECE = DK // LINE
TILES = DV // 128
SLICE = PIECE * TILES
SENT = SLICE + 8
STATE = LINE * SLICE
PER_STEP = 2

f32 = jnp.float32
bf16 = jnp.bfloat16


def triangle():
    rows = lax.broadcasted_iota(jnp.int32, (ROWS, ROWS), 0)
    cols = lax.broadcasted_iota(jnp.int32, (ROWS, ROWS), 1)
    return rows >= cols


def running_of(decay):
    ones = triangle().astype(f32).astype(bf16)
    return lax.dot_general(ones, decay, (((1,), (1,)), ((), ())), preferred_element_type=f32)


def running_rows(decay):
    ones = triangle().astype(f32).astype(bf16)
    return lax.dot_general(decay, ones, (((1,), (1,)), ((), ())), preferred_element_type=f32)


def column(table, head):
    lanes = lax.broadcasted_iota(jnp.int32, table.shape, 1)
    return jnp.sum(jnp.where(lanes == head, table, 0.0), axis=1, keepdims=True)


def put_slices(ref, at, state):
    for o in range(LINE):
        for t in range(TILES):
            ref[at * LINE + o, t * PIECE : (t + 1) * PIECE, :] = state[
                o * PIECE : (o + 1) * PIECE, t * 128 : (t + 1) * 128
            ]


def get_slices(ref, at):
    cols = [
        ref[at * LINE : (at + 1) * LINE, t * PIECE : (t + 1) * PIECE, :].reshape(DK, 128)
        for t in range(TILES)
    ]
    return jnp.concatenate(cols, axis=1)


def state_kernel(group_ref, key_ref, value_ref, decay_ref, out_ref, fade_ref):
    step = pl.program_id(0)

    @pl.when(step == 0)
    def _():
        run = running_of(decay_ref[...])
        fade_ref[...] = jnp.exp(run[ROWS - 1 : ROWS, :] - run)

    for n in range(PER_STEP):
        fade = column(fade_ref[...], group_ref[0] + step * PER_STEP + n)
        faded = (key_ref[:, n * DK : (n + 1) * DK].astype(f32) * fade).astype(bf16)
        state = lax.dot_general(
            faded, value_ref[:, n * DV : (n + 1) * DV], (((0,), (0,)), ((), ())),
            preferred_element_type=f32,
        )
        put_slices(out_ref, n, state.astype(bf16))


def split_rows(damping):
    rows = lax.broadcasted_iota(jnp.int32, (8, 128), 0)
    high = damping.astype(bf16).astype(f32)
    rest = damping - high
    middle = rest.astype(bf16).astype(f32)
    parts = jnp.where(rows == 0, high, jnp.where(rows == 1, middle, rest - middle))
    return parts.astype(bf16)


def joined_row(rows):
    parts = rows.astype(f32)
    return parts[0:1] + parts[1:2] + parts[2:3]


def combine_kernel(group_ref, own_ref, got_ref, decay_ref, other_ref, out_ref, rate_ref):
    step = pl.program_id(0)
    is_first = group_ref[0] < HALF

    @pl.when(step == 0)
    def _():
        ones = jnp.ones((128, ROWS), f32).astype(bf16)
        total = lax.dot_general(
            decay_ref[...], ones, (((1,), (1,)), ((), ())), preferred_element_type=f32
        )
        other = lax.dot_general(
            other_ref[...], ones, (((1,), (1,)), ((), ())), preferred_element_type=f32
        )
        rate_ref[0] = jnp.exp(jnp.where(is_first, other, 0.0))
        rate_ref[1] = jnp.exp(jnp.where(is_first, 0.0, total))
        rate_ref[2] = jnp.exp(total + other)

    for n in range(PER_STEP):
        head = pl.ds(group_ref[0] + step * PER_STEP + n, 1)
        own_rate = rate_ref[0, head, :]
        got_rate = rate_ref[1, head, :]
        for s in range(LINE):
            at = n * LINE + s
            both = own_ref[at].astype(f32) * own_rate + got_ref[at].astype(f32) * got_rate
            out_ref[n, s * SLICE : (s + 1) * SLICE, :] = both.astype(bf16)
        out_ref[n, STATE:, :] = split_rows(rate_ref[2, head, :])


def line_kernel(y_ref, in_ref, *refs):
    outs, total_ref = refs[:LINE], refs[LINE]
    damping = [joined_row(in_ref[z, STATE:, :]) for z in range(LINE)]
    for s in range(LINE):
        rows = slice(s * SLICE, (s + 1) * SLICE)
        state = in_ref[0, rows, :].astype(f32)
        for z in range(1, LINE):
            state = damping[z] * state + in_ref[z, rows, :].astype(f32)
        total_ref[s] = state
    parts = split_rows(damping[0] * damping[1] * damping[2] * damping[3])
    for d in range(LINE):
        outs[d][:SLICE, :] = total_ref[(y_ref[0] + d) % LINE].astype(bf16)
        outs[d][SLICE:, :] = parts


def plane_kernel(y_ref, *refs):
    ins, out_ref, lines_ref = refs[:LINE], refs[LINE], refs[LINE + 1]
    for d in range(LINE):
        lines_ref[(y_ref[0] - d) % LINE] = ins[d][...].astype(f32)
    state = jnp.zeros((SLICE, 128), f32)
    damping = jnp.ones((1, 128), f32)
    for y in range(LINE):
        rate = joined_row(lines_ref[y, SLICE:, :])
        state = rate * state + lines_ref[y, :SLICE, :]
        damping = damping * rate
    out_ref[:SLICE, :] = state.astype(bf16)
    out_ref[SLICE:, :] = split_rows(damping)


def carry_kernel(y_ref, *refs):
    ins, planes, outs = refs[:LINE], refs[LINE : 2 * LINE - 1], refs[2 * LINE - 1 : 3 * LINE - 1]
    lines_ref, carry_ref = refs[3 * LINE - 1 :]
    for d in range(LINE):
        lines_ref[(y_ref[0] - d) % LINE] = ins[d][...].astype(f32)
    state = jnp.zeros((SLICE, 128), f32)
    for plane in reversed(planes):
        state = joined_row(plane[SLICE:, :]) * state + plane[:SLICE, :].astype(f32)
    for y in range(LINE):
        carry_ref[y] = state
        state = joined_row(lines_ref[y, SLICE:, :]) * state + lines_ref[y, :SLICE, :]
    for d in range(LINE):
        outs[d][...] = carry_ref[(y_ref[0] + d) % LINE].astype(bf16)


def start_kernel(y_ref, in_ref, *refs):
    carries, out_ref, carry_ref = refs[:LINE], refs[LINE], refs[LINE + 1]
    for d in range(LINE):
        carry_ref[(y_ref[0] - d) % LINE] = carries[d][...].astype(f32)
    for s in range(LINE):
        rows = slice(s * SLICE, (s + 1) * SLICE)
        state = carry_ref[s]
        for z in range(LINE):
            out_ref[z, rows, :] = state.astype(bf16)
            if z + 1 < LINE:
                state = joined_row(in_ref[z, STATE:, :]) * state + in_ref[z, rows, :].astype(f32)


def within_kernel(group_ref, *refs):
    own, theirs = refs[0:4], refs[4:8]
    decay_ref, other_ref, own_out, theirs_out, reach_out, run_ref, rows_ref, reach_ref = refs[8:]
    step = pl.program_id(0)
    first = group_ref[0]

    @pl.when(step == 0)
    def _():
        run = running_of(decay_ref[...])
        run_ref[...] = run
        rows_ref[...] = running_rows(decay_ref[...])
        other = running_of(other_ref[...])[ROWS - 1 : ROWS, :]
        reach_out[...] = jnp.exp(run + jnp.where(first < HALF, 0.0, other))
        reach_ref[...] = jnp.where(first < HALF, 0.0, jnp.exp(run))

    far = jnp.where(first < HALF, first + HALF, first - HALF)
    for base, ins, out_ref in ((first, own, own_out), (far, theirs, theirs_out)):
        query_ref, key_ref, value_ref, state_ref = ins
        head = base + step
        query = query_ref[...]
        scores = lax.dot_general(
            query, key_ref[...], (((1,), (1,)), ((), ())), preferred_element_type=f32
        )
        spread = column(run_ref[...], head) - rows_ref[pl.ds(head, 1), :]
        factor = jnp.exp(jnp.where(triangle(), spread, -jnp.inf))
        weights = (scores * factor).astype(bf16)
        local = jnp.dot(weights, value_ref[...], preferred_element_type=f32)
        before = jnp.dot(query, get_slices(state_ref, 0), preferred_element_type=f32)
        out_ref[...] = local + before * column(reach_ref[...], head)


def finish_kernel(group_ref, query_ref, start_ref, within_ref, gate_ref, reach_ref, *rest):
    out_ref = rest[-1]
    for n in range(PER_STEP):
        head = group_ref[0] + pl.program_id(0) * PER_STEP + n
        wide = slice(n * DV, (n + 1) * DV)
        across = jnp.dot(
            query_ref[:, n * DK : (n + 1) * DK], get_slices(start_ref, n),
            preferred_element_type=f32,
        )
        retained = within_ref[:, wide] + across * column(reach_ref[...], head)
        average = jnp.mean(retained, axis=1, keepdims=True)
        centered = retained - average
        variance = jnp.mean(centered * centered, axis=1, keepdims=True)
        normed = centered * lax.rsqrt(variance + 1e-06)
        gate = gate_ref[:, wide].astype(f32)
        out_ref[:, wide] = (gate / (1.0 + jnp.exp(-gate)) * normed).astype(bf16)


def call(kernel, name, grid, in_specs, out_specs, out_shape, scratch, flops, aliases=None):
    return pl.pallas_call(
        kernel,
        out_shape=out_shape,
        grid_spec=pltpu.PrefetchScalarGridSpec(
            num_scalar_prefetch=1,
            grid=(grid,),
            in_specs=in_specs,
            out_specs=out_specs,
            scratch_shapes=scratch,
        ),
        compiler_params=pltpu.CompilerParams(dimension_semantics=("arbitrary",)),
        cost_estimate=pl.CostEstimate(flops=flops, transcendentals=0, bytes_accessed=0),
        input_output_aliases=aliases or {},
        name=name,
    )


def shape(*dims, dtype=bf16):
    return jax.ShapeDtypeStruct(dims, dtype)


def exchange(arrays, axis, ring=True):
    done = []
    for d, array in enumerate(arrays, 1):
        pairs = [(i, (i + d) % LINE) for i in range(LINE) if ring or i + d < LINE]
        done.append(lax.ppermute(array, axis, pairs))
    return done


def shards(queries, key_vectors, values, decay_log, gate_input):
    core = lax.axis_index("core").astype(jnp.int32).reshape(1)
    place = lax.axis_index("y").astype(jnp.int32).reshape(1)
    swap = [(0, 1), (1, 0)]
    decay = decay_log.T
    other_decay = lax.ppermute(decay, "core", swap)

    steps = GROUP // PER_STEP
    whole = lambda *dims: pl.BlockSpec(dims, lambda i, c: (0,) * len(dims))
    heads = lambda width, n=PER_STEP: pl.BlockSpec(
        (ROWS, width * n), lambda i, c: (0, c[0] // n + i)
    )
    theirs = lambda width: pl.BlockSpec((ROWS, width), lambda i, c: (0, (c[0] + HALF) % HEADS + i))
    half = lambda width, n=PER_STEP: pl.BlockSpec((ROWS, width * n), lambda i, c: (0, i))
    pieces = lambda n=PER_STEP: pl.BlockSpec((LINE * n, SLICE, 128), lambda i, c: (i, 0, 0))
    decays = whole(HEADS, ROWS)
    table = pltpu.VMEM((ROWS, HEADS), f32)
    flops = 2 * GROUP * ROWS * DK * DV
    slices_shape = shape(GROUP * LINE, SLICE, 128)
    local = pl.BlockSpec(memory_space=pltpu.VMEM)

    def chunk_states(group, name):
        return call(
            state_kernel, name, steps, [heads(DK), heads(DV), decays], pieces(),
            slices_shape, [table], flops,
        )(group, key_vectors, values, decay)

    def within_of(g, their_first, late_decay):
        return call(
            within_kernel, f"within_{g}", GROUP,
            [heads(DK, 1), heads(DK, 1), heads(DV, 1), pieces(1),
             theirs(DK), theirs(DK), theirs(DV), pieces(1), decays, decays],
            [half(DV, 1), half(DV, 1), whole(ROWS, HEADS)],
            [shape(ROWS, GROUP * DV, dtype=f32)] * 2 + [shape(ROWS, HEADS, dtype=f32)],
            [table, pltpu.VMEM((HEADS, ROWS), f32), table], 4 * flops,
        )(own_heads[g], queries, key_vectors, values, got[g], queries, key_vectors, values,
          their_first, late_decay, other_decay)

    def starts_of(g):
        lines = call(
            line_kernel, f"line_{g}", 1, [whole(LINE, STATE + 8, 128)], [local] * LINE,
            [shape(SENT, 128)] * LINE, [pltpu.VMEM((LINE, SLICE, 128), f32)], flops // 16,
        )(place, collected[g])
        lines = [lines[0]] + exchange(lines[1:], "y")
        plane = call(
            plane_kernel, f"plane_{g}", 1, [local] * LINE, local,
            shape(SENT, 128), [pltpu.VMEM((LINE, SENT, 128), f32)], flops // 64,
        )(place, *lines)
        planes = exchange([plane] * (LINE - 1), "x", ring=False)
        carries = call(
            carry_kernel, f"carry_{g}", 1, [local] * (2 * LINE - 1), [local] * LINE,
            [shape(SLICE, 128)] * LINE,
            [pltpu.VMEM((LINE, SENT, 128), f32), pltpu.VMEM((LINE, SLICE, 128), f32)], flops // 64,
        )(place, *lines, *planes)
        carries = [carries[0]] + exchange(carries[1:], "y")
        return call(
            start_kernel, f"starts_{g}", 1, [whole(LINE, STATE + 8, 128)] + [local] * LINE,
            whole(LINE, STATE, 128), shape(LINE, STATE, 128),
            [pltpu.VMEM((LINE, SLICE, 128), f32)], flops // 16,
        )(place, collected[g], *carries)

    own_heads = [core * HALF + g * GROUP for g in range(GROUPS)]
    their_heads = [(1 - core) * HALF + g * GROUP for g in range(GROUPS)]
    collected, got, own_states = [], [], []
    for g in range(GROUPS):
        theirs_state = chunk_states(their_heads[g], f"theirs_state_{g}")
        got.append(lax.ppermute(theirs_state, "core", swap))
        own_states.append(chunk_states(own_heads[g], f"own_state_{g}"))
        block_state = call(
            combine_kernel, f"combine_{g}", steps, [pieces(), pieces(), decays, decays],
            pl.BlockSpec((PER_STEP, STATE + 8, 128), lambda i, c: (i, 0, 0)),
            shape(LINE, STATE + 8, 128), [pltpu.VMEM((3, HEADS, 128), f32)], flops // 8,
        )(own_heads[g], own_states[g], got[g], decay, other_decay)
        collected.append(lax.all_to_all(block_state, "z", 0, 0, tiled=True))

    within = [within_of(g, lax.ppermute(own_states[g], "core", swap), decay) for g in range(GROUPS)]
    start = [
        lax.all_to_all(starts_of(g), "z", 0, 0, tiled=True).reshape(GROUP * LINE, SLICE, 128)
        for g in range(GROUPS)
    ]
    specs = [heads(DK), pieces(), half(DV), heads(DV), whole(ROWS, HEADS)]
    result = shape(ROWS, HEADS * DV)
    done = None
    for g in range(GROUPS):
        their_start = lax.ppermute(start[g], "core", swap)
        for n, (group, states) in enumerate(((own_heads[g], start[g]), (their_heads[g], their_start))):
            more = [] if done is None else [done]
            done = call(
                finish_kernel, f"finish_{g}_{n}", steps,
                specs + [pl.BlockSpec(memory_space=pl.ANY)] * len(more),
                heads(DV), result, [], flops, {6: 0} if more else None,
            )(group, queries, states, within[g][n], gate_input, within[g][2], *more)
    return done


def solution(mesh):
    mesh = Mesh(mesh.devices.reshape(4, 4, 4, 2), ("x", "y", "z", "core"))
    spec = P(("x", "y", "z", "core"), None)
    return jax.shard_map(
        shards, mesh=mesh, in_specs=(spec,) * 5, out_specs=spec, check_vma=False
    )
```

```python
import jax
import jax.numpy as jnp
from jax import lax
from jax.experimental import pallas as pl
from jax.experimental.pallas import tpu as pltpu
from jax.sharding import Mesh, PartitionSpec as P


HEADS = 16
DK = 256
DV = 512
ROWS = 256
HALF = HEADS // 2
CHIPS = 64
SLICES = CHIPS // HALF
PIECE = DK // SLICES
TILES = DV // 128
SLICE = PIECE * TILES
SENT = SLICE + 8
PER_STEP = 4
MIB = 2**20
LIMIT = 20

f32 = jnp.float32
bf16 = jnp.bfloat16


def triangle():
    rows = lax.broadcasted_iota(jnp.int32, (ROWS, ROWS), 0)
    cols = lax.broadcasted_iota(jnp.int32, (ROWS, ROWS), 1)
    return rows >= cols


def running_of(decay):
    ones = triangle().astype(f32).astype(bf16)
    return lax.dot_general(ones, decay, (((1,), (1,)), ((), ())), preferred_element_type=f32)


def running_rows(decay):
    ones = triangle().astype(f32).astype(bf16)
    return lax.dot_general(decay, ones, (((1,), (1,)), ((), ())), preferred_element_type=f32)


def column(table, head):
    lanes = lax.broadcasted_iota(jnp.int32, table.shape, 1)
    return jnp.sum(jnp.where(lanes == head, table, 0.0), axis=1, keepdims=True)


def put_slices(ref, at, state):
    for o in range(SLICES):
        for t in range(TILES):
            ref[at * SLICES + o, t * PIECE : (t + 1) * PIECE, :] = state[
                o * PIECE : (o + 1) * PIECE, t * 128 : (t + 1) * 128
            ]


def get_slices(ref, at):
    cols = [
        ref[pl.ds(at * SLICES, SLICES), t * PIECE : (t + 1) * PIECE, :].reshape(DK, 128)
        for t in range(TILES)
    ]
    return jnp.concatenate(cols, axis=1)


def state_kernel(group_ref, key_ref, value_ref, decay_ref, *refs):
    if len(refs) == 2:
        (out_ref, fade_ref), copies = refs, ()
    else:
        done_ref, out_ref, copy_ref, done_copy_ref, fade_ref = refs
        copies = (copy_ref,)
        size = PER_STEP * SLICES
        done_copy_ref[...] = done_ref[pl.ds(pl.program_id(0) * size, size)]
    step = pl.program_id(0)

    @pl.when(step == 0)
    def _():
        run = running_of(decay_ref[...])
        fade_ref[...] = jnp.exp(run[ROWS - 1 : ROWS, :] - run)

    for n in range(PER_STEP):
        at = step * PER_STEP + n
        fade = column(fade_ref[...], group_ref[0] * HALF + at)
        faded = (key_ref[:, n * DK : (n + 1) * DK].astype(f32) * fade).astype(bf16)
        state = lax.dot_general(
            faded, value_ref[:, n * DV : (n + 1) * DV], (((0,), (0,)), ((), ())),
            preferred_element_type=f32,
        )
        put_slices(out_ref, at, state.astype(bf16))
        for copy_ref in copies:
            put_slices(copy_ref, n, state.astype(bf16))


def combine_kernel(core_ref, own_ref, got_ref, decay_ref, other_ref, out_ref, rate_ref):
    step = pl.program_id(0)
    is_first = core_ref[0] == 0
    ones = jnp.ones((128, ROWS), f32).astype(bf16)
    total = lax.dot_general(
        decay_ref[...], ones, (((1,), (1,)), ((), ())), preferred_element_type=f32
    )
    other = lax.dot_general(
        other_ref[...], ones, (((1,), (1,)), ((), ())), preferred_element_type=f32
    )
    rate_ref[0] = jnp.exp(jnp.where(is_first, other, 0.0))
    rate_ref[1] = jnp.exp(jnp.where(is_first, 0.0, total))
    rate_ref[2] = jnp.exp(total + other)
    rows = lax.broadcasted_iota(jnp.int32, (8, 128), 0)
    for n in range(PER_STEP):
        head = pl.ds(core_ref[0] * HALF + step * PER_STEP + n, 1)
        own_rate = rate_ref[0, head, :]
        got_rate = rate_ref[1, head, :]
        damping = rate_ref[2, head, :]
        high = damping.astype(bf16).astype(f32)
        rest = damping - high
        middle = rest.astype(bf16).astype(f32)
        parts = jnp.where(rows == 0, high, jnp.where(rows == 1, middle, rest - middle))
        parts = parts.astype(bf16)
        for o in range(n * SLICES, (n + 1) * SLICES):
            at = step * PER_STEP * SLICES + o
            both = own_ref[at].astype(f32) * own_rate + got_ref[at].astype(f32) * got_rate
            out_ref[o, :SLICE, :] = both.astype(bf16)
            out_ref[o, SLICE:SENT, :] = parts


def within_kernel(core_ref, *refs):
    own, theirs, (got_ref, first_ref, decay_ref, other_ref) = refs[0:4], refs[4:8], refs[8:12]
    outs, (reach_out, run_ref, rows_ref, reach_ref) = refs[12:16], refs[16:]
    step = pl.program_id(0)
    core = core_ref[0]

    @pl.when(step == 0)
    def _():
        run = running_of(decay_ref[...])
        run_ref[...] = run
        rows_ref[...] = running_rows(decay_ref[...])
        other = running_of(other_ref[...])[ROWS - 1 : ROWS, :]
        reach = jnp.exp(run + jnp.where(core == 0, 0.0, other))
        for h in range(HEADS):
            reach_out[h] = jnp.broadcast_to(reach[:, h : h + 1], (ROWS, 128))
        reach_ref[...] = jnp.where(core == 0, 0.0, jnp.exp(run))

    for group, ins, state_ref, out_ref, gated_ref in (
        (core, own, got_ref, outs[0], outs[1]),
        (1 - core, theirs, first_ref, outs[2], outs[3]),
    ):
        query_ref, key_ref, value_ref, gate_ref = ins
        head = group * HALF + step
        query = query_ref[...]
        scores = lax.dot_general(
            query, key_ref[...], (((1,), (1,)), ((), ())), preferred_element_type=f32
        )
        spread = column(run_ref[...], head) - rows_ref[pl.ds(head, 1), :]
        factor = jnp.exp(jnp.where(triangle(), spread, -jnp.inf))
        weights = (scores * factor).astype(bf16)
        local = jnp.dot(weights, value_ref[...], preferred_element_type=f32)
        before = jnp.dot(query, get_slices(state_ref, 0), preferred_element_type=f32)
        out_ref[0] = local + before * column(reach_ref[...], head)
        gate = gate_ref[...].astype(f32)
        gated_ref[0] = gate / (1.0 + jnp.exp(-gate))


def prefix_kernel(in_ref, out_ref):
    state = jnp.zeros((SLICE, 128), f32)
    for b in range(CHIPS):
        parts = in_ref[b, SLICE:SENT, :].astype(f32)
        damping = parts[0:1] + parts[1:2] + parts[2:3]
        out_ref[b] = state.astype(bf16)
        state = damping * state + in_ref[b, :SLICE, :].astype(f32)


def finish_kernel(group_ref, query_ref, start_ref, within_ref, gated_ref, reach_ref, *rest):
    out_ref = rest[-1]
    for n in range(PER_STEP):
        at = pl.program_id(0) * PER_STEP + n
        across = jnp.dot(
            query_ref[:, n * DK : (n + 1) * DK], get_slices(start_ref, at),
            preferred_element_type=f32,
        )
        reach = reach_ref[n]
        retained = within_ref[n] + across * jnp.concatenate([reach] * TILES, axis=1)
        average = jnp.mean(retained, axis=1, keepdims=True)
        centered = retained - average
        variance = jnp.mean(centered * centered, axis=1, keepdims=True)
        normed = centered * lax.rsqrt(variance + 1e-06)
        out_ref[:, n * DV : (n + 1) * DV] = (gated_ref[n] * normed).astype(bf16)


def call(kernel, grid, in_specs, out_specs, out_shape, scratch, flops, aliases=None):
    return pl.pallas_call(
        kernel,
        out_shape=out_shape,
        grid_spec=pltpu.PrefetchScalarGridSpec(
            num_scalar_prefetch=1,
            grid=(grid,),
            in_specs=in_specs,
            out_specs=out_specs,
            scratch_shapes=scratch,
        ),
        compiler_params=pltpu.CompilerParams(
            dimension_semantics=("arbitrary",), vmem_limit_bytes=LIMIT * MIB
        ),
        cost_estimate=pl.CostEstimate(flops=flops, transcendentals=0, bytes_accessed=0),
        input_output_aliases=aliases or {},
    )


def far(value):
    return pltpu.with_memory_space_constraint(value, pltpu.HBM)


def near(value):
    return pltpu.with_memory_space_constraint(value, pltpu.VMEM)


def shape(*dims, dtype=bf16):
    return jax.ShapeDtypeStruct(dims, dtype)


def shards(queries, key_vectors, values, decay_log, gate_input):
    core = lax.axis_index("core").astype(jnp.int32).reshape(1)
    other = 1 - core
    swap = [(0, 1), (1, 0)]
    everyone = ("seq", "chip")
    decay = decay_log.T
    other_decay = lax.ppermute(decay, "core", swap)

    steps = HALF // PER_STEP
    here = pl.BlockSpec(memory_space=pltpu.VMEM)
    decays = pl.BlockSpec((HEADS, ROWS), lambda i, c: (0, 0))
    heads = lambda width, n=PER_STEP: pl.BlockSpec(
        (ROWS, width * n), lambda i, c: (0, c[0] * (HALF // n) + i)
    )
    theirs = lambda width: pl.BlockSpec((ROWS, width), lambda i, c: (0, (1 - c[0]) * HALF + i))
    table = pltpu.VMEM((ROWS, HEADS), f32)
    flops = 2 * HALF * ROWS * DK * DV
    slices = pltpu.VMEM((CHIPS, SLICE, 128), bf16)

    pieces = pl.BlockSpec((SLICES * PER_STEP, SLICE, 128), lambda i, c: (i, 0, 0))
    sent = pl.BlockSpec((SLICES * PER_STEP, SENT, 128), lambda i, c: (i, 0, 0))
    key_far, value_far, decay_far = far(key_vectors), far(values), far(decay)

    def chunk_states(group, out_specs, out_shape, *done):
        return call(
            state_kernel, steps, [heads(DK), heads(DV), decays] + [here] * len(done),
            out_specs, out_shape, [table], flops,
        )(group, key_far, value_far, decay_far, *done)

    theirs_state = chunk_states(other, here, slices)
    got = lax.ppermute(theirs_state, "core", swap)
    stored = pltpu.HBM((CHIPS, SLICE, 128), bf16)
    own_state, late_own, late_theirs = chunk_states(
        core, [here, pieces, pieces], [slices, stored, stored], near(theirs_state)
    )
    block_state = call(
        combine_kernel, steps, [here, here, decays, decays], sent,
        pltpu.HBM((CHIPS, SENT, 128), bf16), [pltpu.VMEM((3, HEADS, 128), f32)], flops // 8,
    )(core, near(own_state), near(got), decay_far, other_decay)
    collected = lax.all_to_all(block_state, everyone, 0, 0, tiled=True)
    their_first = lax.ppermute(late_own, "core", swap)
    own_first = lax.ppermute(late_theirs, "core", swap)

    block = lambda: pl.BlockSpec((1, ROWS, DV), lambda i, c: (i, 0, 0))
    own_within, own_gated, their_within, their_gated, reach = call(
        within_kernel, HALF,
        [heads(DK, 1), heads(DK, 1), heads(DV, 1), heads(DV, 1),
         theirs(DK), theirs(DK), theirs(DV), theirs(DV),
         pl.BlockSpec((SLICES, SLICE, 128), lambda i, c: (i, 0, 0)),
         pl.BlockSpec((SLICES, SLICE, 128), lambda i, c: (i, 0, 0)), decays, decays],
        [block() for _ in range(4)] + [pl.BlockSpec((HEADS, ROWS, 128), lambda i, c: (0, 0, 0))],
        [pltpu.HBM((HALF, ROWS, DV), f32)] * 4 + [pltpu.HBM((HEADS, ROWS, 128), f32)],
        [table, pltpu.VMEM((HEADS, ROWS), f32), table], 4 * flops,
    )(core, far(queries), key_far, value_far, far(gate_input), far(queries), key_far, value_far,
      far(gate_input), far(own_first), far(their_first), decay_far, other_decay)

    starts = pl.pallas_call(
        prefix_kernel,
        out_shape=slices,
        in_specs=[here],
        out_specs=here,
        compiler_params=pltpu.CompilerParams(vmem_limit_bytes=LIMIT * MIB),
        name="prefix",
    )(near(collected))
    start = lax.all_to_all(starts, everyone, 0, 0, tiled=True)
    their_start = lax.ppermute(start, "core", swap)

    blocks = pl.BlockSpec((PER_STEP, ROWS, DV), lambda i, c: (i, 0, 0))
    reaches = pl.BlockSpec((PER_STEP, ROWS, 128), lambda i, c: (c[0] * steps + i, 0, 0))
    specs = [heads(DK), here, blocks, blocks, reaches]
    result = shape(ROWS, HEADS * DV)
    done = call(finish_kernel, steps, specs, heads(DV), result, [], flops)(
        core, far(queries), near(start), far(own_within), far(own_gated), far(reach)
    )
    return call(
        finish_kernel, steps, specs + [pl.BlockSpec(memory_space=pl.ANY)],
        heads(DV), result, [], flops, {6: 0},
    )(other, far(queries), near(their_start), far(their_within), far(their_gated), far(reach), done)


def solution(mesh):
    mesh = Mesh(mesh.devices.reshape(4, 16, 2), ("seq", "chip", "core"))
    spec = P(("seq", "chip", "core"), None)

    return jax.shard_map(shards, mesh=mesh, in_specs=(spec,) * 5, out_specs=spec, check_vma=False)
```

```python
import jax
import jax.numpy as jnp
from jax import lax
from jax.experimental import pallas as pl
from jax.experimental.pallas import tpu as pltpu
from jax.sharding import Mesh, PartitionSpec as P


HEADS = 16
DK = 256
DV = 512
ROWS = 256
HALF = HEADS // 2
CHIPS = 64
SLICES = CHIPS // HALF
PIECE = DK // SLICES
TILES = DV // 128
SLICE = PIECE * TILES
SENT = SLICE + 8
MIB = 2**20
LIMIT = 20

f32 = jnp.float32
bf16 = jnp.bfloat16


def triangle():
    rows = lax.broadcasted_iota(jnp.int32, (ROWS, ROWS), 0)
    cols = lax.broadcasted_iota(jnp.int32, (ROWS, ROWS), 1)
    return rows >= cols


def running_of(decay):
    ones = triangle().astype(f32).astype(bf16)
    return lax.dot_general(ones, decay, (((1,), (1,)), ((), ())), preferred_element_type=f32)


def running_rows(decay):
    ones = triangle().astype(f32).astype(bf16)
    return lax.dot_general(decay, ones, (((1,), (1,)), ((), ())), preferred_element_type=f32)


def column(table, head):
    lanes = lax.broadcasted_iota(jnp.int32, table.shape, 1)
    return jnp.sum(jnp.where(lanes == head, table, 0.0), axis=1, keepdims=True)


def put_slices(ref, at, state):
    for o in range(SLICES):
        for t in range(TILES):
            ref[at * SLICES + o, t * PIECE : (t + 1) * PIECE, :] = state[
                o * PIECE : (o + 1) * PIECE, t * 128 : (t + 1) * 128
            ]


def get_slices(ref, at):
    cols = [
        ref[pl.ds(at * SLICES, SLICES), t * PIECE : (t + 1) * PIECE, :].reshape(DK, 128)
        for t in range(TILES)
    ]
    return jnp.concatenate(cols, axis=1)


def columns_of(ref, head, width):
    return ref.at[:, pl.ds(pl.multiple_of(head * width, width), width)]


def start_all(copies):
    for copy in copies:
        copy.start()
    return copies


def states_into(out_ref, group, key_ref, value_ref, run, key_buf, value_buf, sems, done=None):
    copies = []
    for n in range(HALF):
        head = group * HALF + n
        copies.append(start_all((
            pltpu.make_async_copy(columns_of(key_ref, head, DK), key_buf.at[n], sems.at[0, n]),
            pltpu.make_async_copy(columns_of(value_ref, head, DV), value_buf.at[n], sems.at[1, n]),
        )))
    fades = jnp.exp(run[ROWS - 1 : ROWS, :] - run)
    for n in range(HALF):
        fade = column(fades, group * HALF + n)
        for copy in copies[n]:
            copy.wait()
        faded = (key_buf[n].astype(f32) * fade).astype(bf16)
        state = lax.dot_general(
            faded, value_buf[n], (((0,), (0,)), ((), ())), preferred_element_type=f32
        )
        put_slices(out_ref, n, state.astype(bf16))
        if done is not None:
            done(n)


def totals_of(decay):
    ones = jnp.ones((128, ROWS), f32).astype(bf16)
    return lax.dot_general(decay, ones, (((1,), (1,)), ((), ())), preferred_element_type=f32)


def thirds_of(value):
    high = value.astype(bf16).astype(f32)
    rest = value - high
    middle = rest.astype(bf16).astype(f32)
    return high, middle, rest - middle


def theirs_kernel(group_ref, key_ref, value_ref, decay_ref, out_ref, key_buf, value_buf, sems):
    run = running_of(decay_ref[...])
    states_into(out_ref, group_ref[0], key_ref, value_ref, run, key_buf, value_buf, sems)
    for k, third in enumerate(thirds_of(totals_of(decay_ref[...]))):
        out_ref[CHIPS, k * HEADS : (k + 1) * HEADS, :] = third.astype(bf16)


def own_kernel(
    group_ref, key_ref, value_ref, decay_ref, theirs_ref,
    out_ref, total_ref, own_copy_ref, theirs_copy_ref, key_buf, value_buf, sems, out_sems,
):
    theirs_copy = pltpu.make_async_copy(
        theirs_ref.at[pl.ds(0, CHIPS)], theirs_copy_ref, out_sems.at[HALF]
    )
    theirs_copy.start()
    decay = decay_ref[...]
    total_ref[...] = totals_of(decay)
    copies = []

    def done(n):
        rows = pl.ds(n * SLICES, SLICES)
        copies.extend(start_all((
            pltpu.make_async_copy(out_ref.at[rows], own_copy_ref.at[rows], out_sems.at[n]),
        )))

    states_into(
        out_ref, group_ref[0], key_ref, value_ref, running_of(decay), key_buf, value_buf, sems, done
    )
    theirs_copy.wait()
    for copy in copies:
        copy.wait()


def combine_kernel(core_ref, own_ref, got_ref, total_ref, out_ref, buf_ref, rate_ref, sems):
    is_first = core_ref[0] == 0
    total = total_ref[...]
    thirds = [got_ref[CHIPS, k * HEADS : (k + 1) * HEADS, :].astype(f32) for k in range(3)]
    other = thirds[0] + thirds[1] + thirds[2]
    rate_ref[0] = jnp.exp(jnp.where(is_first, other, 0.0))
    rate_ref[1] = jnp.exp(jnp.where(is_first, 0.0, total))
    rate_ref[2] = jnp.exp(total + other)
    rows = lax.broadcasted_iota(jnp.int32, (8, 128), 0)
    copies = []
    for n in range(HALF):
        head = pl.ds(core_ref[0] * HALF + n, 1)
        own_rate = rate_ref[0, head, :]
        got_rate = rate_ref[1, head, :]
        high, middle, low = thirds_of(rate_ref[2, head, :])
        parts = jnp.where(rows == 0, high, jnp.where(rows == 1, middle, low))
        parts = parts.astype(bf16)
        for o in range(n * SLICES, (n + 1) * SLICES):
            both = own_ref[o].astype(f32) * own_rate + got_ref[o].astype(f32) * got_rate
            buf_ref[o, :SLICE, :] = both.astype(bf16)
            buf_ref[o, SLICE:SENT, :] = parts
        block = pl.ds(n * SLICES, SLICES)
        copies.extend(start_all((
            pltpu.make_async_copy(buf_ref.at[block], out_ref.at[block], sems.at[n]),
        )))
    for copy in copies:
        copy.wait()


def within_kernel(core_ref, *refs):
    own, theirs, (got_ref, first_ref, decay_ref, other_ref) = refs[0:3], refs[3:6], refs[6:10]
    outs, (reach_out, run_ref, rows_ref, reach_ref) = refs[10:12], refs[12:]
    step = pl.program_id(0)
    core = core_ref[0]

    @pl.when(step == 0)
    def _():
        run = running_of(decay_ref[...])
        run_ref[...] = run
        rows_ref[...] = running_rows(decay_ref[...])
        other = running_of(other_ref[...])[ROWS - 1 : ROWS, :]
        reach = jnp.exp(run + jnp.where(core == 0, 0.0, other))
        reach_out[...] = reach
        reach_ref[...] = jnp.where(core == 0, 0.0, jnp.exp(run))

    for group, ins, state_ref, out_ref in (
        (core, own, got_ref, outs[0]),
        (1 - core, theirs, first_ref, outs[1]),
    ):
        query_ref, key_ref, value_ref = ins
        head = group * HALF + step
        query = query_ref[...]
        scores = lax.dot_general(
            query, key_ref[...], (((1,), (1,)), ((), ())), preferred_element_type=f32
        )
        spread = column(run_ref[...], head) - rows_ref[pl.ds(head, 1), :]
        factor = jnp.exp(jnp.where(triangle(), spread, -jnp.inf))
        weights = (scores * factor).astype(bf16)
        local = jnp.dot(weights, value_ref[...], preferred_element_type=f32)
        before = jnp.dot(query, get_slices(state_ref, 0), preferred_element_type=f32)
        out_ref[0] = local + before * column(reach_ref[...], head)


def prefix_kernel(in_ref, out_ref):
    state = jnp.zeros((SLICE, 128), f32)
    for b in range(CHIPS):
        parts = in_ref[b, SLICE:SENT, :].astype(f32)
        damping = parts[0:1] + parts[1:2] + parts[2:3]
        out_ref[b] = state.astype(bf16)
        state = damping * state + in_ref[b, :SLICE, :].astype(f32)


def finish_kernel(group_ref, start_ref, reach_ref, query_ref, within_ref, gate_ref, *rest):
    out_ref, query_buf, within_buf, gate_buf, out_buf, sems = rest[-6:]
    copies, writes = [], []
    for n in range(HALF):
        head = group_ref[0] * HALF + n
        copies.append(start_all((
            pltpu.make_async_copy(columns_of(query_ref, head, DK), query_buf.at[n], sems.at[0, n]),
            pltpu.make_async_copy(within_ref.at[n], within_buf.at[n], sems.at[1, n]),
            pltpu.make_async_copy(columns_of(gate_ref, head, DV), gate_buf.at[n], sems.at[2, n]),
        )))
    for n in range(HALF):
        head = group_ref[0] * HALF + n
        reach = column(reach_ref[...], head)
        for copy in copies[n]:
            copy.wait()
        across = jnp.dot(query_buf[n], get_slices(start_ref, n), preferred_element_type=f32)
        retained = within_buf[n] + across * reach
        average = jnp.mean(retained, axis=1, keepdims=True)
        centered = retained - average
        variance = jnp.mean(centered * centered, axis=1, keepdims=True)
        normed = centered * lax.rsqrt(variance + 1e-06)
        gate = gate_buf[n].astype(f32)
        out_buf[n] = (gate / (1.0 + jnp.exp(-gate)) * normed).astype(bf16)
        writes.extend(start_all((
            pltpu.make_async_copy(out_buf.at[n], columns_of(out_ref, head, DV), sems.at[3, n]),
        )))
    for copy in writes:
        copy.wait()


def call(kernel, grid, in_specs, out_specs, out_shape, scratch, flops, aliases=None):
    return pl.pallas_call(
        kernel,
        out_shape=out_shape,
        grid_spec=pltpu.PrefetchScalarGridSpec(
            num_scalar_prefetch=1,
            grid=(grid,),
            in_specs=in_specs,
            out_specs=out_specs,
            scratch_shapes=scratch,
        ),
        compiler_params=pltpu.CompilerParams(
            dimension_semantics=("arbitrary",), vmem_limit_bytes=LIMIT * MIB
        ),
        cost_estimate=pl.CostEstimate(flops=flops, transcendentals=0, bytes_accessed=0),
        input_output_aliases=aliases or {},
    )


def far(value):
    return pltpu.with_memory_space_constraint(value, pltpu.HBM)


def near(value):
    return pltpu.with_memory_space_constraint(value, pltpu.VMEM)


def shards(queries, key_vectors, values, decay_log, gate_input):
    core = lax.axis_index("core").astype(jnp.int32).reshape(1)
    other = 1 - core
    swap = [(0, 1), (1, 0)]
    everyone = ("seq", "chip")
    decay = decay_log.T

    here = pl.BlockSpec(memory_space=pltpu.VMEM)
    decays = pl.BlockSpec((HEADS, ROWS), lambda i, c: (0, 0))
    heads = lambda width: pl.BlockSpec((ROWS, width), lambda i, c: (0, c[0] * HALF + i))
    theirs = lambda width: pl.BlockSpec((ROWS, width), lambda i, c: (0, (1 - c[0]) * HALF + i))
    table = pltpu.VMEM((ROWS, HEADS), f32)
    flops = 2 * HALF * ROWS * DK * DV
    slices = pltpu.VMEM((CHIPS, SLICE, 128), bf16)

    away = pl.BlockSpec(memory_space=pl.ANY)
    key_far, value_far, decay_far = far(key_vectors), far(values), far(decay)
    stored = pltpu.HBM((CHIPS, SLICE, 128), bf16)
    buffers = [
        pltpu.VMEM((HALF, ROWS, DK), bf16), pltpu.VMEM((HALF, ROWS, DV), bf16),
        pltpu.SemaphoreType.DMA((2, HALF)),
    ]
    theirs_state = call(
        theirs_kernel, 1, [away, away, decays], here,
        pltpu.VMEM((CHIPS + 1, SLICE, 128), bf16), buffers, flops
    )(other, key_far, value_far, decay_far)
    got = lax.ppermute(theirs_state, "core", swap)
    own_state, totals, late_own, late_theirs = call(
        own_kernel, 1, [away, away, decays, here], [here, here, away, away],
        [slices, pltpu.VMEM((HEADS, 128), f32), stored, stored],
        buffers + [pltpu.SemaphoreType.DMA((HALF + 1,))], flops,
    )(core, key_far, value_far, decay_far, near(theirs_state))
    block_state = call(
        combine_kernel, 1, [here, here, here], away,
        pltpu.HBM((CHIPS, SENT, 128), bf16),
        [
            pltpu.VMEM((CHIPS, SENT, 128), bf16), pltpu.VMEM((3, HEADS, 128), f32),
            pltpu.SemaphoreType.DMA((HALF,)),
        ], flops // 8,
    )(core, near(own_state), near(got), near(totals))
    collected = lax.all_to_all(block_state, everyone, 0, 0, tiled=True)
    their_first = lax.ppermute(late_own, "core", swap)
    own_first = lax.ppermute(late_theirs, "core", swap)
    other_decay = lax.ppermute(decay, "core", swap)

    block = lambda: pl.BlockSpec((1, ROWS, DV), lambda i, c: (i, 0, 0))
    own_within, their_within, reach = call(
        within_kernel, HALF,
        [heads(DK), heads(DK), heads(DV), theirs(DK), theirs(DK), theirs(DV),
         pl.BlockSpec((SLICES, SLICE, 128), lambda i, c: (i, 0, 0)),
         pl.BlockSpec((SLICES, SLICE, 128), lambda i, c: (i, 0, 0)), decays, decays],
        [block(), block(), pl.BlockSpec((ROWS, HEADS), lambda i, c: (0, 0))],
        [pltpu.HBM((HALF, ROWS, DV), f32)] * 2 + [pltpu.HBM((ROWS, HEADS), f32)],
        [table, pltpu.VMEM((HEADS, ROWS), f32), table], 4 * flops,
    )(core, far(queries), key_far, value_far, far(queries), key_far, value_far,
      far(own_first), far(their_first), decay_far, other_decay)

    starts = pl.pallas_call(
        prefix_kernel,
        out_shape=slices,
        in_specs=[here],
        out_specs=here,
        compiler_params=pltpu.CompilerParams(vmem_limit_bytes=LIMIT * MIB),
        name="prefix",
    )(near(collected))
    start = lax.all_to_all(starts, everyone, 0, 0, tiled=True)
    their_start = lax.ppermute(start, "core", swap)

    specs = [here, pl.BlockSpec((ROWS, HEADS), lambda i, c: (0, 0)), away, away, away]
    result = pltpu.HBM((ROWS, HEADS * DV), bf16)
    scratch = [
        pltpu.VMEM((HALF, ROWS, DK), bf16), pltpu.VMEM((HALF, ROWS, DV), f32),
        pltpu.VMEM((HALF, ROWS, DV), bf16), pltpu.VMEM((HALF, ROWS, DV), bf16),
        pltpu.SemaphoreType.DMA((4, HALF)),
    ]
    done = call(finish_kernel, 1, specs, away, result, scratch, flops)(
        core, near(start), far(reach), far(queries), far(own_within), far(gate_input)
    )
    return call(
        finish_kernel, 1, specs + [away], away, result, scratch, flops, {6: 0},
    )(other, near(their_start), far(reach), far(queries), far(their_within), far(gate_input), done)


def solution(mesh):
    mesh = Mesh(mesh.devices.reshape(4, 16, 2), ("seq", "chip", "core"))
    spec = P(("seq", "chip", "core"), None)

    return jax.shard_map(shards, mesh=mesh, in_specs=(spec,) * 5, out_specs=spec, check_vma=False)
```

```python
from functools import partial

import jax
import jax.numpy as jnp
from jax import lax
from jax.experimental import pallas as pl
from jax.experimental.pallas import tpu as pltpu
from jax.sharding import Mesh, PartitionSpec as P


HEADS = 16
DK = 256
DV = 512
ROWS = 256
HALF = HEADS // 2
CHIPS = 64
SLICES = CHIPS // HALF
PIECE = DK // SLICES
TILES = DV // 128
SLICE = PIECE * TILES
SENT = SLICE + 8
PER_STEP = 4
MIB = 2**20
LIMIT = 20

f32 = jnp.float32
bf16 = jnp.bfloat16


def triangle():
    rows = lax.broadcasted_iota(jnp.int32, (ROWS, ROWS), 0)
    cols = lax.broadcasted_iota(jnp.int32, (ROWS, ROWS), 1)
    return rows >= cols


def running_of(decay):
    ones = triangle().astype(f32).astype(bf16)
    return lax.dot_general(ones, decay, (((1,), (1,)), ((), ())), preferred_element_type=f32)


def running_rows(decay):
    ones = triangle().astype(f32).astype(bf16)
    return lax.dot_general(decay, ones, (((1,), (1,)), ((), ())), preferred_element_type=f32)


def column(table, head):
    lanes = lax.broadcasted_iota(jnp.int32, table.shape, 1)
    return jnp.sum(jnp.where(lanes == head, table, 0.0), axis=1, keepdims=True)


def put_slices(ref, at, state):
    for o in range(SLICES):
        for t in range(TILES):
            ref[at * SLICES + o, t * PIECE : (t + 1) * PIECE, :] = state[
                o * PIECE : (o + 1) * PIECE, t * 128 : (t + 1) * 128
            ]


def get_slices(ref, at):
    cols = [
        ref[pl.ds(at * SLICES, SLICES), t * PIECE : (t + 1) * PIECE, :].reshape(DK, 128)
        for t in range(TILES)
    ]
    return jnp.concatenate(cols, axis=1)


def start_all(copies):
    for copy in copies:
        copy.start()
    return copies


def states_into(refs, group, step, key_ref, value_ref, fade_ref):
    for n in range(PER_STEP):
        at = step * PER_STEP + n
        fade = column(fade_ref[...], group * HALF + at)
        faded = (key_ref[:, n * DK : (n + 1) * DK].astype(f32) * fade).astype(bf16)
        state = lax.dot_general(
            faded, value_ref[:, n * DV : (n + 1) * DV], (((0,), (0,)), ((), ())),
            preferred_element_type=f32,
        ).astype(bf16)
        for ref, place in zip(refs, (at, n)):
            put_slices(ref, place, state)


def fades_of(decay):
    run = running_of(decay)
    return jnp.exp(run[ROWS - 1 : ROWS, :] - run)


def totals_of(decay):
    ones = jnp.ones((128, ROWS), f32).astype(bf16)
    return lax.dot_general(decay, ones, (((1,), (1,)), ((), ())), preferred_element_type=f32)


def thirds_of(value):
    high = value.astype(bf16).astype(f32)
    rest = value - high
    middle = rest.astype(bf16).astype(f32)
    return high, middle, rest - middle


def theirs_kernel(group_ref, key_ref, value_ref, decay_ref, out_ref, fade_ref):
    step = pl.program_id(0)

    @pl.when(step == 0)
    def _():
        fade_ref[...] = fades_of(decay_ref[...])
        for k, third in enumerate(thirds_of(totals_of(decay_ref[...]))):
            out_ref[CHIPS, k * HEADS : (k + 1) * HEADS, :] = third.astype(bf16)

    states_into((out_ref,), group_ref[0], step, key_ref, value_ref, fade_ref)


def own_kernel(
    group_ref, key_ref, value_ref, decay_ref, theirs_ref,
    out_ref, total_ref, own_copy_ref, theirs_copy_ref, fade_ref,
):
    step = pl.program_id(0)

    @pl.when(step == 0)
    def _():
        fade_ref[...] = fades_of(decay_ref[...])
        total_ref[...] = totals_of(decay_ref[...])

    size = PER_STEP * SLICES
    theirs_copy_ref[...] = theirs_ref[pl.ds(step * size, size)]
    states_into((out_ref, own_copy_ref), group_ref[0], step, key_ref, value_ref, fade_ref)


def combine_kernel(core_ref, own_ref, got_ref, total_ref, out_ref, buf_ref, rate_ref, sems):
    is_first = core_ref[0] == 0
    total = total_ref[...]
    thirds = [got_ref[CHIPS, k * HEADS : (k + 1) * HEADS, :].astype(f32) for k in range(3)]
    other = thirds[0] + thirds[1] + thirds[2]
    rate_ref[0] = jnp.exp(jnp.where(is_first, other, 0.0))
    rate_ref[1] = jnp.exp(jnp.where(is_first, 0.0, total))
    rate_ref[2] = jnp.exp(total + other)
    rows = lax.broadcasted_iota(jnp.int32, (8, 128), 0)
    copies = []
    for n in range(HALF):
        head = pl.ds(core_ref[0] * HALF + n, 1)
        own_rate = rate_ref[0, head, :]
        got_rate = rate_ref[1, head, :]
        high, middle, low = thirds_of(rate_ref[2, head, :])
        parts = jnp.where(rows == 0, high, jnp.where(rows == 1, middle, low))
        parts = parts.astype(bf16)
        for o in range(n * SLICES, (n + 1) * SLICES):
            both = own_ref[o].astype(f32) * own_rate + got_ref[o].astype(f32) * got_rate
            buf_ref[o, :SLICE, :] = both.astype(bf16)
            buf_ref[o, SLICE:SENT, :] = parts
        block = pl.ds(n * SLICES, SLICES)
        copies.extend(start_all((
            pltpu.make_async_copy(buf_ref.at[block], out_ref.at[block], sems.at[n]),
        )))
    for copy in copies:
        copy.wait()


def within_kernel(core_ref, *refs):
    own, theirs, (got_ref, first_ref, decay_ref, other_ref) = refs[0:3], refs[3:6], refs[6:10]
    out_ref, reach_out, run_ref, rows_ref, reach_ref = refs[10:]
    step = pl.program_id(0)
    core = core_ref[0]

    @pl.when(step == 0)
    def _():
        run = running_of(decay_ref[...])
        run_ref[...] = run
        rows_ref[...] = running_rows(decay_ref[...])
        other = running_of(other_ref[...])[ROWS - 1 : ROWS, :]
        reach = jnp.exp(run + jnp.where(core == 0, 0.0, other))
        reach_out[...] = reach
        reach_ref[...] = jnp.where(core == 0, 0.0, jnp.exp(run))

    for side, (group, ins, state_ref) in enumerate((
        (core, own, got_ref), (1 - core, theirs, first_ref),
    )):
        query_ref, key_ref, value_ref = ins
        head = group * HALF + step
        query = query_ref[...]
        scores = lax.dot_general(
            query, key_ref[...], (((1,), (1,)), ((), ())), preferred_element_type=f32
        )
        spread = column(run_ref[...], head) - rows_ref[pl.ds(head, 1), :]
        factor = jnp.exp(jnp.where(triangle(), spread, -jnp.inf))
        weights = (scores * factor).astype(bf16)
        local = jnp.dot(weights, value_ref[...], preferred_element_type=f32)
        before = jnp.dot(query, get_slices(state_ref, 0), preferred_element_type=f32)
        out_ref[side, 0] = local + before * column(reach_ref[...], head)


def prefix_kernel(in_ref, out_ref):
    state = jnp.zeros((SLICE, 128), f32)
    for b in range(CHIPS):
        parts = in_ref[b, SLICE:SENT, :].astype(f32)
        damping = parts[0:1] + parts[1:2] + parts[2:3]
        out_ref[b] = state.astype(bf16)
        state = damping * state + in_ref[b, :SLICE, :].astype(f32)


def finish_kernel(side, group_ref, start_ref, reach_ref, query_ref, within_ref, gate_ref, *rest):
    out_ref = rest[-1]
    for n in range(PER_STEP):
        at = pl.program_id(0) * PER_STEP + n
        head = group_ref[0] * HALF + at
        across = jnp.dot(query_ref[:, n * DK : (n + 1) * DK], get_slices(start_ref, at), preferred_element_type=f32)
        retained = within_ref[side, at] + across * column(reach_ref[...], head)
        average = jnp.mean(retained, axis=1, keepdims=True)
        centered = retained - average
        variance = jnp.mean(centered * centered, axis=1, keepdims=True)
        normed = centered * lax.rsqrt(variance + 1e-06)
        gate = 0.5 * gate_ref[:, n * DV : (n + 1) * DV].astype(f32)
        out_ref[:, n * DV : (n + 1) * DV] = ((gate + gate * jnp.tanh(gate)) * normed).astype(bf16)


def call(kernel, grid, in_specs, out_specs, out_shape, scratch, flops, aliases=None):
    return pl.pallas_call(
        kernel,
        out_shape=out_shape,
        grid_spec=pltpu.PrefetchScalarGridSpec(
            num_scalar_prefetch=1,
            grid=(grid,),
            in_specs=in_specs,
            out_specs=out_specs,
            scratch_shapes=scratch,
        ),
        compiler_params=pltpu.CompilerParams(
            dimension_semantics=("arbitrary",), vmem_limit_bytes=LIMIT * MIB
        ),
        cost_estimate=pl.CostEstimate(flops=flops, transcendentals=0, bytes_accessed=0),
        input_output_aliases=aliases or {},
    )


def far(value):
    return pltpu.with_memory_space_constraint(value, pltpu.HBM)


def near(value):
    return pltpu.with_memory_space_constraint(value, pltpu.VMEM)


def shards(queries, key_vectors, values, decay_log, gate_input):
    core = lax.axis_index("core").astype(jnp.int32).reshape(1)
    other = 1 - core
    swap = [(0, 1), (1, 0)]
    everyone = ("seq", "chip")
    decay = decay_log.T

    steps = HALF // PER_STEP
    here = pl.BlockSpec(memory_space=pltpu.VMEM)
    decays = pl.BlockSpec((HEADS, ROWS), lambda i, c: (0, 0))
    heads = lambda width: pl.BlockSpec((ROWS, width), lambda i, c: (0, c[0] * HALF + i))
    theirs = lambda width: pl.BlockSpec((ROWS, width), lambda i, c: (0, (1 - c[0]) * HALF + i))
    table = pltpu.VMEM((ROWS, HEADS), f32)
    flops = 2 * HALF * ROWS * DK * DV
    slices = pltpu.VMEM((CHIPS, SLICE, 128), bf16)

    away = pl.BlockSpec(memory_space=pl.ANY)
    key_far, value_far, decay_far = far(key_vectors), far(values), far(decay)
    stored = pltpu.HBM((CHIPS, SLICE, 128), bf16)
    wide = lambda width: pl.BlockSpec(
        (ROWS, width * PER_STEP), lambda i, c: (0, c[0] * steps + i)
    )
    pieces = pl.BlockSpec((SLICES * PER_STEP, SLICE, 128), lambda i, c: (i, 0, 0))
    theirs_state = call(
        theirs_kernel, steps, [wide(DK), wide(DV), decays], here,
        pltpu.VMEM((CHIPS + 1, SLICE, 128), bf16), [table], flops
    )(other, key_far, value_far, decay_far)
    got = lax.ppermute(theirs_state, "core", swap)
    own_state, totals, late_own, late_theirs = call(
        own_kernel, steps, [wide(DK), wide(DV), decays, here],
        [here, here, pieces, pieces],
        [slices, pltpu.VMEM((HEADS, 128), f32), stored, stored],
        [table], flops,
    )(core, key_far, value_far, decay_far, near(theirs_state))
    block_state = call(
        combine_kernel, 1, [here, here, here], away,
        pltpu.HBM((CHIPS, SENT, 128), bf16),
        [
            pltpu.VMEM((CHIPS, SENT, 128), bf16), pltpu.VMEM((3, HEADS, 128), f32),
            pltpu.SemaphoreType.DMA((HALF,)),
        ], flops // 8,
    )(core, near(own_state), near(got), near(totals))
    collected = lax.all_to_all(block_state, everyone, 0, 0, tiled=True)
    their_first = lax.ppermute(late_own, "core", swap)
    own_first = lax.ppermute(late_theirs, "core", swap)
    other_decay = lax.ppermute(decay, "core", swap)

    block = pl.BlockSpec((2, 1, ROWS, DV), lambda i, c: (0, i, 0, 0))
    within, reach = call(
        within_kernel, HALF,
        [heads(DK), heads(DK), heads(DV), theirs(DK), theirs(DK), theirs(DV),
         pl.BlockSpec((SLICES, SLICE, 128), lambda i, c: (i, 0, 0)),
         pl.BlockSpec((SLICES, SLICE, 128), lambda i, c: (i, 0, 0)), decays, decays],
        [block, pl.BlockSpec((ROWS, HEADS), lambda i, c: (0, 0))],
        [pltpu.HBM((2, HALF, ROWS, DV), f32), pltpu.HBM((ROWS, HEADS), f32)],
        [table, pltpu.VMEM((HEADS, ROWS), f32), table], 4 * flops,
    )(core, far(queries), key_far, value_far, far(queries), key_far, value_far,
      far(own_first), far(their_first), decay_far, other_decay)

    starts = pl.pallas_call(
        prefix_kernel,
        out_shape=slices,
        in_specs=[here],
        out_specs=here,
        compiler_params=pltpu.CompilerParams(vmem_limit_bytes=LIMIT * MIB),
        name="prefix",
    )(near(collected))
    start = lax.all_to_all(starts, everyone, 0, 0, tiled=True)
    their_start = lax.ppermute(start, "core", swap)

    specs = [
        here, pl.BlockSpec((ROWS, HEADS), lambda i, c: (0, 0)),
        wide(DK),
        here,
        wide(DV),
    ]
    result = pltpu.HBM((ROWS, HEADS * DV), bf16)
    done = call(partial(finish_kernel, 0), steps, specs, wide(DV), result, [], flops)(
        core, near(start), far(reach), far(queries), near(within), far(gate_input)
    )
    return call(
        partial(finish_kernel, 1), steps, specs + [away], wide(DV), result, [], flops, {6: 0},
    )(other, near(their_start), far(reach), far(queries), near(within), far(gate_input), done)


def solution(mesh):
    mesh = Mesh(mesh.devices.reshape(4, 16, 2), ("seq", "chip", "core"))
    spec = P(("seq", "chip", "core"), None)

    return jax.shard_map(shards, mesh=mesh, in_specs=(spec,) * 5, out_specs=spec, check_vma=False)
```

```python
from functools import partial

import jax
import jax.numpy as jnp
from jax import lax
from jax.experimental import pallas as pl
from jax.experimental.pallas import tpu as pltpu
from jax.sharding import Mesh, PartitionSpec as P


HEADS = 16
DK = 256
DV = 512
ROWS = 256
HALF = HEADS // 2
CHIPS = 64
SLICES = CHIPS // HALF
PIECE = DK // SLICES
TILES = DV // 128
SLICE = PIECE * TILES
SENT = SLICE + 8
PER_STEP = 4
MIB = 2**20
LIMIT = 20

f32 = jnp.float32
bf16 = jnp.bfloat16


def triangle():
    rows = lax.broadcasted_iota(jnp.int32, (ROWS, ROWS), 0)
    cols = lax.broadcasted_iota(jnp.int32, (ROWS, ROWS), 1)
    return rows >= cols


def running_of(decay):
    ones = triangle().astype(f32).astype(bf16)
    return lax.dot_general(ones, decay, (((1,), (1,)), ((), ())), preferred_element_type=f32)


def running_rows(decay):
    ones = triangle().astype(f32).astype(bf16)
    return lax.dot_general(decay, ones, (((1,), (1,)), ((), ())), preferred_element_type=f32)


def column(table, head):
    lanes = lax.broadcasted_iota(jnp.int32, table.shape, 1)
    return jnp.sum(jnp.where(lanes == head, table, 0.0), axis=1, keepdims=True)


def put_slices(ref, at, state):
    for o in range(SLICES):
        for t in range(TILES):
            ref[at * SLICES + o, t * PIECE : (t + 1) * PIECE, :] = state[
                o * PIECE : (o + 1) * PIECE, t * 128 : (t + 1) * 128
            ]


def get_slices(ref, at):
    cols = [
        ref[pl.ds(at * SLICES, SLICES), t * PIECE : (t + 1) * PIECE, :].reshape(DK, 128)
        for t in range(TILES)
    ]
    return jnp.concatenate(cols, axis=1)


def start_all(copies):
    for copy in copies:
        copy.start()
    return copies


def states_into(refs, group, step, key_ref, value_ref, fade_ref):
    for n in range(PER_STEP):
        at = step * PER_STEP + n
        fade = column(fade_ref[...], group * HALF + at)
        faded = (key_ref[:, n * DK : (n + 1) * DK].astype(f32) * fade).astype(bf16)
        state = lax.dot_general(
            faded, value_ref[:, n * DV : (n + 1) * DV], (((0,), (0,)), ((), ())),
            preferred_element_type=f32,
        ).astype(bf16)
        for ref, place in zip(refs, (at, n)):
            put_slices(ref, place, state)


def fades_of(decay):
    run = running_of(decay)
    return jnp.exp(run[ROWS - 1 : ROWS, :] - run)


def totals_of(decay):
    ones = jnp.ones((128, ROWS), f32).astype(bf16)
    return lax.dot_general(decay, ones, (((1,), (1,)), ((), ())), preferred_element_type=f32)


def thirds_of(value):
    high = value.astype(bf16).astype(f32)
    rest = value - high
    middle = rest.astype(bf16).astype(f32)
    return high, middle, rest - middle


def theirs_kernel(group_ref, key_ref, value_ref, decay_ref, out_ref, fade_ref):
    step = pl.program_id(0)

    @pl.when(step == 0)
    def _():
        fade_ref[...] = fades_of(decay_ref[...])
        for k, third in enumerate(thirds_of(totals_of(decay_ref[...]))):
            out_ref[CHIPS, k * HEADS : (k + 1) * HEADS, :] = third.astype(bf16)

    states_into((out_ref,), group_ref[0], step, key_ref, value_ref, fade_ref)


def own_kernel(
    group_ref, key_ref, value_ref, decay_ref, theirs_ref,
    out_ref, total_ref, own_copy_ref, theirs_copy_ref, fade_ref,
):
    step = pl.program_id(0)

    @pl.when(step == 0)
    def _():
        fade_ref[...] = fades_of(decay_ref[...])
        total_ref[...] = totals_of(decay_ref[...])

    size = PER_STEP * SLICES
    theirs_copy_ref[...] = theirs_ref[pl.ds(step * size, size)]
    states_into((out_ref, own_copy_ref), group_ref[0], step, key_ref, value_ref, fade_ref)


def combine_kernel(core_ref, own_ref, got_ref, total_ref, out_ref, buf_ref, rate_ref, sems):
    is_first = core_ref[0] == 0
    total = total_ref[...]
    thirds = [got_ref[CHIPS, k * HEADS : (k + 1) * HEADS, :].astype(f32) for k in range(3)]
    other = thirds[0] + thirds[1] + thirds[2]
    rate_ref[0] = jnp.exp(jnp.where(is_first, other, 0.0))
    rate_ref[1] = jnp.exp(jnp.where(is_first, 0.0, total))
    rate_ref[2] = jnp.exp(total + other)
    rows = lax.broadcasted_iota(jnp.int32, (8, 128), 0)
    copies = []
    for n in range(HALF):
        head = pl.ds(core_ref[0] * HALF + n, 1)
        own_rate = rate_ref[0, head, :]
        got_rate = rate_ref[1, head, :]
        high, middle, low = thirds_of(rate_ref[2, head, :])
        parts = jnp.where(rows == 0, high, jnp.where(rows == 1, middle, low))
        parts = parts.astype(bf16)
        for o in range(n * SLICES, (n + 1) * SLICES):
            both = own_ref[o].astype(f32) * own_rate + got_ref[o].astype(f32) * got_rate
            buf_ref[o, :SLICE, :] = both.astype(bf16)
            buf_ref[o, SLICE:SENT, :] = parts
        block = pl.ds(n * SLICES, SLICES)
        copies.extend(start_all((
            pltpu.make_async_copy(buf_ref.at[block], out_ref.at[block], sems.at[n]),
        )))
    for copy in copies:
        copy.wait()


def within_kernel(core_ref, *refs):
    own, theirs, (got_ref, first_ref, decay_ref, other_ref) = refs[0:4], refs[4:8], refs[8:12]
    out_ref, reach_out, run_ref, rows_ref, reach_ref = refs[12:]
    step = pl.program_id(0)
    core = core_ref[0]

    @pl.when(step == 0)
    def _():
        run = running_of(decay_ref[...])
        run_ref[...] = run
        rows_ref[...] = running_rows(decay_ref[...])
        other = running_of(other_ref[...])[ROWS - 1 : ROWS, :]
        reach = jnp.exp(run + jnp.where(core == 0, 0.0, other))
        reach_out[...] = reach
        reach_ref[...] = jnp.where(core == 0, 0.0, jnp.exp(run))

    for side, (group, ins, state_ref) in enumerate((
        (core, own, got_ref), (1 - core, theirs, first_ref),
    )):
        query_ref, key_ref, value_ref, gate_ref = ins
        head = group * HALF + step
        query = query_ref[...]
        scores = lax.dot_general(
            query, key_ref[...], (((1,), (1,)), ((), ())), preferred_element_type=f32
        )
        spread = column(run_ref[...], head) - rows_ref[pl.ds(head, 1), :]
        factor = jnp.exp(jnp.where(triangle(), spread, -jnp.inf))
        weights = (scores * factor).astype(bf16)
        local = jnp.dot(weights, value_ref[...], preferred_element_type=f32)
        before = jnp.dot(query, get_slices(state_ref, step), preferred_element_type=f32)
        inner = local + before * column(reach_ref[...], head)
        out_ref[side, 0, :, :DV] = inner.astype(bf16)
        gate = 0.5 * gate_ref[...].astype(f32)
        out_ref[side, 0, :, DV:] = (gate + gate * jnp.tanh(gate)).astype(bf16)


def prefix_kernel(in_ref, out_ref):
    state = jnp.zeros((SLICE, 128), f32)
    for b in range(CHIPS):
        parts = in_ref[b, SLICE:SENT, :].astype(f32)
        damping = parts[0:1] + parts[1:2] + parts[2:3]
        out_ref[b] = state.astype(bf16)
        state = damping * state + in_ref[b, :SLICE, :].astype(f32)


def finish_kernel(side, group_ref, start_ref, reach_ref, query_ref, ready_ref, *rest):
    out_ref = rest[-1]
    for n in range(PER_STEP):
        at = pl.program_id(0) * PER_STEP + n
        across = jnp.dot(
            query_ref[:, n * DK : (n + 1) * DK], get_slices(start_ref, at),
            preferred_element_type=f32,
        )
        reach = column(reach_ref[...], group_ref[0] * HALF + at)
        retained = ready_ref[side, at, :, :DV].astype(f32) + across * reach
        average = jnp.mean(retained, axis=1, keepdims=True)
        centered = retained - average
        variance = jnp.mean(centered * centered, axis=1, keepdims=True)
        normed = centered * lax.rsqrt(variance + 1e-06)
        gated = ready_ref[side, at, :, DV:].astype(f32)
        out_ref[:, n * DV : (n + 1) * DV] = (gated * normed).astype(bf16)


def call(kernel, grid, in_specs, out_specs, out_shape, scratch, flops, aliases=None):
    return pl.pallas_call(
        kernel,
        out_shape=out_shape,
        grid_spec=pltpu.PrefetchScalarGridSpec(
            num_scalar_prefetch=1,
            grid=(grid,),
            in_specs=in_specs,
            out_specs=out_specs,
            scratch_shapes=scratch,
        ),
        compiler_params=pltpu.CompilerParams(
            dimension_semantics=("arbitrary",), vmem_limit_bytes=LIMIT * MIB
        ),
        cost_estimate=pl.CostEstimate(flops=flops, transcendentals=0, bytes_accessed=0),
        input_output_aliases=aliases or {},
    )


def far(value):
    return pltpu.with_memory_space_constraint(value, pltpu.HBM)


def near(value):
    return pltpu.with_memory_space_constraint(value, pltpu.VMEM)


def shards(queries, key_vectors, values, decay_log, gate_input):
    core = lax.axis_index("core").astype(jnp.int32).reshape(1)
    other = 1 - core
    swap = [(0, 1), (1, 0)]
    everyone = ("seq", "chip")
    decay = decay_log.T

    steps = HALF // PER_STEP
    here = pl.BlockSpec(memory_space=pltpu.VMEM)
    decays = pl.BlockSpec((HEADS, ROWS), lambda i, c: (0, 0))
    heads = lambda width: pl.BlockSpec((ROWS, width), lambda i, c: (0, c[0] * HALF + i))
    theirs = lambda width: pl.BlockSpec((ROWS, width), lambda i, c: (0, (1 - c[0]) * HALF + i))
    table = pltpu.VMEM((ROWS, HEADS), f32)
    flops = 2 * HALF * ROWS * DK * DV
    slices = pltpu.VMEM((CHIPS, SLICE, 128), bf16)

    away = pl.BlockSpec(memory_space=pl.ANY)
    key_far, value_far, decay_far = far(key_vectors), far(values), far(decay)
    stored = pltpu.HBM((CHIPS, SLICE, 128), bf16)
    wide = lambda width: pl.BlockSpec(
        (ROWS, width * PER_STEP), lambda i, c: (0, c[0] * steps + i)
    )
    pieces = pl.BlockSpec((SLICES * PER_STEP, SLICE, 128), lambda i, c: (i, 0, 0))
    theirs_state = call(
        theirs_kernel, steps, [wide(DK), wide(DV), decays], here,
        pltpu.VMEM((CHIPS + 1, SLICE, 128), bf16), [table], flops
    )(other, key_far, value_far, decay_far)
    got = lax.ppermute(theirs_state, "core", swap)
    own_state, totals, late_own, late_theirs = call(
        own_kernel, steps, [wide(DK), wide(DV), decays, here],
        [here, here, pieces, pieces],
        [slices, pltpu.VMEM((HEADS, 128), f32), stored, stored],
        [table], flops,
    )(core, key_far, value_far, decay_far, near(theirs_state))
    block_state = call(
        combine_kernel, 1, [here, here, here], away,
        pltpu.HBM((CHIPS, SENT, 128), bf16),
        [
            pltpu.VMEM((CHIPS, SENT, 128), bf16), pltpu.VMEM((3, HEADS, 128), f32),
            pltpu.SemaphoreType.DMA((HALF,)),
        ], flops // 8,
    )(core, near(own_state), near(got), near(totals))
    collected = lax.all_to_all(block_state, everyone, 0, 0, tiled=True)
    their_first = lax.ppermute(late_own, "core", swap)
    own_first = lax.ppermute(late_theirs, "core", swap)
    other_decay = lax.ppermute(decay, "core", swap)

    block = pl.BlockSpec((2, 1, ROWS, 2 * DV), lambda i, c: (0, i, 0, 0))
    within, reach = call(
        within_kernel, HALF,
        [heads(DK), heads(DK), heads(DV), heads(DV),
         theirs(DK), theirs(DK), theirs(DV), theirs(DV), here, here, decays, decays],
        [block, pl.BlockSpec((ROWS, HEADS), lambda i, c: (0, 0))],
        [pltpu.HBM((2, HALF, ROWS, 2 * DV), bf16), pltpu.HBM((ROWS, HEADS), f32)],
        [table, pltpu.VMEM((HEADS, ROWS), f32), table], 4 * flops,
    )(core, far(queries), key_far, value_far, far(gate_input), far(queries), key_far, value_far,
      far(gate_input), near(own_first), near(their_first), decay_far, other_decay)

    starts = pl.pallas_call(
        prefix_kernel,
        out_shape=slices,
        in_specs=[here],
        out_specs=here,
        compiler_params=pltpu.CompilerParams(vmem_limit_bytes=LIMIT * MIB),
        name="prefix",
    )(near(collected))
    start = lax.all_to_all(starts, everyone, 0, 0, tiled=True)
    their_start = lax.ppermute(start, "core", swap)

    specs = [here, pl.BlockSpec((ROWS, HEADS), lambda i, c: (0, 0)), wide(DK), here]
    result = pltpu.HBM((ROWS, HEADS * DV), bf16)
    done = call(partial(finish_kernel, 0), steps, specs, wide(DV), result, [], flops)(
        core, near(start), far(reach), far(queries), near(within)
    )
    return call(
        partial(finish_kernel, 1), steps, specs + [away], wide(DV), result, [], flops, {5: 0},
    )(other, near(their_start), far(reach), far(queries), near(within), done)


def solution(mesh):
    mesh = Mesh(mesh.devices.reshape(4, 16, 2), ("seq", "chip", "core"))
    spec = P(("seq", "chip", "core"), None)

    return jax.shard_map(shards, mesh=mesh, in_specs=(spec,) * 5, out_specs=spec, check_vma=False)
```

```python
from functools import partial

import jax
import jax.numpy as jnp
from jax import lax
from jax.experimental import pallas as pl
from jax.experimental.pallas import tpu as pltpu
from jax.sharding import Mesh, PartitionSpec as P


HEADS = 16
DK = 256
DV = 512
ROWS = 256
HALF = HEADS // 2
CHIPS = 64
SLICES = CHIPS // HALF
PIECE = DK // SLICES
TILES = DV // 128
SLICE = PIECE * TILES
SENT = SLICE + 8
PER_STEP = 4
MIB = 2**20
LIMIT = 20

f32 = jnp.float32
bf16 = jnp.bfloat16


def triangle():
    rows = lax.broadcasted_iota(jnp.int32, (ROWS, ROWS), 0)
    cols = lax.broadcasted_iota(jnp.int32, (ROWS, ROWS), 1)
    return rows >= cols


def running_of(decay):
    ones = triangle().astype(f32).astype(bf16)
    return lax.dot_general(ones, decay, (((1,), (1,)), ((), ())), preferred_element_type=f32)


def running_rows(decay):
    ones = triangle().astype(f32).astype(bf16)
    return lax.dot_general(decay, ones, (((1,), (1,)), ((), ())), preferred_element_type=f32)


def column(table, head):
    lanes = lax.broadcasted_iota(jnp.int32, table.shape, 1)
    return jnp.sum(jnp.where(lanes == head, table, 0.0), axis=1, keepdims=True)


def put_slices(ref, at, state):
    for o in range(SLICES):
        for t in range(TILES):
            ref[at * SLICES + o, t * PIECE : (t + 1) * PIECE, :] = state[
                o * PIECE : (o + 1) * PIECE, t * 128 : (t + 1) * 128
            ]


def get_slices(ref, at):
    cols = [
        ref[pl.ds(at * SLICES, SLICES), t * PIECE : (t + 1) * PIECE, :].reshape(DK, 128)
        for t in range(TILES)
    ]
    return jnp.concatenate(cols, axis=1)


def start_all(copies):
    for copy in copies:
        copy.start()
    return copies


def states_into(refs, group, step, key_ref, value_ref, fade_ref):
    for n in range(PER_STEP):
        at = step * PER_STEP + n
        fade = column(fade_ref[...], group * HALF + at)
        faded = (key_ref[:, n * DK : (n + 1) * DK].astype(f32) * fade).astype(bf16)
        state = lax.dot_general(
            faded, value_ref[:, n * DV : (n + 1) * DV], (((0,), (0,)), ((), ())),
            preferred_element_type=f32,
        ).astype(bf16)
        for ref, place in zip(refs, (at, n)):
            put_slices(ref, place, state)


def fades_of(decay):
    run = running_of(decay)
    return jnp.exp(run[ROWS - 1 : ROWS, :] - run)


def totals_of(decay):
    ones = jnp.ones((128, ROWS), f32).astype(bf16)
    return lax.dot_general(decay, ones, (((1,), (1,)), ((), ())), preferred_element_type=f32)


def thirds_of(value):
    high = value.astype(bf16).astype(f32)
    rest = value - high
    middle = rest.astype(bf16).astype(f32)
    return high, middle, rest - middle


def theirs_kernel(group_ref, key_ref, value_ref, decay_ref, out_ref, fade_ref):
    step = pl.program_id(0)

    @pl.when(step == 0)
    def _():
        fade_ref[...] = fades_of(decay_ref[...])
        for k, third in enumerate(thirds_of(totals_of(decay_ref[...]))):
            out_ref[CHIPS, k * HEADS : (k + 1) * HEADS, :] = third.astype(bf16)

    states_into((out_ref,), group_ref[0], step, key_ref, value_ref, fade_ref)


def own_kernel(
    group_ref, key_ref, value_ref, decay_ref, theirs_ref,
    out_ref, total_ref, own_copy_ref, theirs_copy_ref, fade_ref,
):
    step = pl.program_id(0)

    @pl.when(step == 0)
    def _():
        fade_ref[...] = fades_of(decay_ref[...])
        total_ref[...] = totals_of(decay_ref[...])

    size = PER_STEP * SLICES
    theirs_copy_ref[...] = theirs_ref[pl.ds(step * size, size)]
    states_into((out_ref, own_copy_ref), group_ref[0], step, key_ref, value_ref, fade_ref)


def combine_kernel(core_ref, own_ref, got_ref, total_ref, out_ref, buf_ref, rate_ref, sems):
    is_first = core_ref[0] == 0
    total = total_ref[...]
    thirds = [got_ref[CHIPS, k * HEADS : (k + 1) * HEADS, :].astype(f32) for k in range(3)]
    other = thirds[0] + thirds[1] + thirds[2]
    rate_ref[0] = jnp.exp(jnp.where(is_first, other, 0.0))
    rate_ref[1] = jnp.exp(jnp.where(is_first, 0.0, total))
    rate_ref[2] = jnp.exp(total + other)
    rows = lax.broadcasted_iota(jnp.int32, (8, 128), 0)
    copies = []
    for n in range(HALF):
        head = pl.ds(core_ref[0] * HALF + n, 1)
        own_rate = rate_ref[0, head, :]
        got_rate = rate_ref[1, head, :]
        high, middle, low = thirds_of(rate_ref[2, head, :])
        parts = jnp.where(rows == 0, high, jnp.where(rows == 1, middle, low))
        parts = parts.astype(bf16)
        for o in range(n * SLICES, (n + 1) * SLICES):
            both = own_ref[o].astype(f32) * own_rate + got_ref[o].astype(f32) * got_rate
            buf_ref[o, :SLICE, :] = both.astype(bf16)
            buf_ref[o, SLICE:SENT, :] = parts
        block = pl.ds(n * SLICES, SLICES)
        copies.extend(start_all((
            pltpu.make_async_copy(buf_ref.at[block], out_ref.at[block], sems.at[n]),
        )))
    for copy in copies:
        copy.wait()


def within_kernel(core_ref, *refs):
    own, theirs, (got_ref, first_ref, decay_ref, other_ref) = refs[0:4], refs[4:8], refs[8:12]
    out_ref, reach_out, run_ref, rows_ref, reach_ref = refs[12:]
    step = pl.program_id(0)
    core = core_ref[0]

    @pl.when(step == 0)
    def _():
        run = running_of(decay_ref[...])
        run_ref[...] = run
        rows_ref[...] = running_rows(decay_ref[...])
        other = running_of(other_ref[...])[ROWS - 1 : ROWS, :]
        reach = jnp.exp(run + jnp.where(core == 0, 0.0, other))
        reach_out[...] = reach
        reach_ref[...] = jnp.where(core == 0, 0.0, jnp.exp(run))

    for side, (group, ins, state_ref) in enumerate((
        (core, own, got_ref), (1 - core, theirs, first_ref),
    )):
        query_ref, key_ref, value_ref, gate_ref = ins
        head = group * HALF + step
        query = query_ref[...]
        scores = lax.dot_general(
            query, key_ref[...], (((1,), (1,)), ((), ())), preferred_element_type=f32
        )
        spread = column(run_ref[...], head) - rows_ref[pl.ds(head, 1), :]
        factor = jnp.exp(jnp.where(triangle(), spread, -jnp.inf))
        weights = (scores * factor).astype(bf16)
        local = jnp.dot(weights, value_ref[...], preferred_element_type=f32)
        before = jnp.dot(query, get_slices(state_ref, step), preferred_element_type=f32)
        inner = local + before * column(reach_ref[...], head)
        out_ref[side, 0, :, :DV] = inner
        gate = 0.5 * gate_ref[...].astype(f32)
        out_ref[side, 0, :, DV:] = gate + gate * jnp.tanh(gate)


def prefix_kernel(in_ref, out_ref):
    state = jnp.zeros((SLICE, 128), f32)
    for b in range(CHIPS):
        parts = in_ref[b, SLICE:SENT, :].astype(f32)
        damping = parts[0:1] + parts[1:2] + parts[2:3]
        out_ref[b] = state.astype(bf16)
        state = damping * state + in_ref[b, :SLICE, :].astype(f32)


def finish_kernel(side, group_ref, start_ref, reach_ref, query_ref, ready_ref, *rest):
    out_ref = rest[-1]
    for n in range(PER_STEP):
        at = pl.program_id(0) * PER_STEP + n
        head = group_ref[0] * HALF + at
        across = jnp.dot(
            query_ref[:, pl.ds(pl.multiple_of(head * DK, DK), DK)], get_slices(start_ref, at),
            preferred_element_type=f32,
        )
        reach = column(reach_ref[...], head)
        retained = ready_ref[side, at, :, :DV] + across * reach
        average = jnp.mean(retained, axis=1, keepdims=True)
        centered = retained - average
        variance = jnp.mean(centered * centered, axis=1, keepdims=True)
        normed = centered * lax.rsqrt(variance + 1e-06)
        gated = ready_ref[side, at, :, DV:]
        out_ref[:, n * DV : (n + 1) * DV] = (gated * normed).astype(bf16)


def call(kernel, grid, in_specs, out_specs, out_shape, scratch, flops, aliases=None):
    return pl.pallas_call(
        kernel,
        out_shape=out_shape,
        grid_spec=pltpu.PrefetchScalarGridSpec(
            num_scalar_prefetch=1,
            grid=(grid,),
            in_specs=in_specs,
            out_specs=out_specs,
            scratch_shapes=scratch,
        ),
        compiler_params=pltpu.CompilerParams(
            dimension_semantics=("arbitrary",), vmem_limit_bytes=LIMIT * MIB
        ),
        cost_estimate=pl.CostEstimate(flops=flops, transcendentals=0, bytes_accessed=0),
        input_output_aliases=aliases or {},
    )


def far(value):
    return pltpu.with_memory_space_constraint(value, pltpu.HBM)


def near(value):
    return pltpu.with_memory_space_constraint(value, pltpu.VMEM)


def shards(queries, key_vectors, values, decay_log, gate_input):
    core = lax.axis_index("core").astype(jnp.int32).reshape(1)
    other = 1 - core
    swap = [(0, 1), (1, 0)]
    everyone = ("seq", "chip")
    decay = decay_log.T

    steps = HALF // PER_STEP
    here = pl.BlockSpec(memory_space=pltpu.VMEM)
    decays = pl.BlockSpec((HEADS, ROWS), lambda i, c: (0, 0))
    heads = lambda width: pl.BlockSpec((ROWS, width), lambda i, c: (0, c[0] * HALF + i))
    theirs = lambda width: pl.BlockSpec((ROWS, width), lambda i, c: (0, (1 - c[0]) * HALF + i))
    table = pltpu.VMEM((ROWS, HEADS), f32)
    flops = 2 * HALF * ROWS * DK * DV
    slices = pltpu.VMEM((CHIPS, SLICE, 128), bf16)

    away = pl.BlockSpec(memory_space=pl.ANY)
    key_far, value_far, decay_far = far(key_vectors), far(values), far(decay)
    stored = pltpu.HBM((CHIPS, SLICE, 128), bf16)
    wide = lambda width: pl.BlockSpec(
        (ROWS, width * PER_STEP), lambda i, c: (0, c[0] * steps + i)
    )
    pieces = pl.BlockSpec((SLICES * PER_STEP, SLICE, 128), lambda i, c: (i, 0, 0))
    theirs_state = call(
        theirs_kernel, steps, [wide(DK), wide(DV), decays], here,
        pltpu.VMEM((CHIPS + 1, SLICE, 128), bf16), [table], flops
    )(other, key_far, value_far, decay_far)
    got = lax.ppermute(theirs_state, "core", swap)
    own_state, totals, late_own, late_theirs = call(
        own_kernel, steps, [wide(DK), wide(DV), decays, here],
        [here, here, pieces, pieces],
        [slices, pltpu.VMEM((HEADS, 128), f32), stored, stored],
        [table], flops,
    )(core, key_far, value_far, decay_far, near(theirs_state))
    block_state = call(
        combine_kernel, 1, [here, here, here], away,
        pltpu.HBM((CHIPS, SENT, 128), bf16),
        [
            pltpu.VMEM((CHIPS, SENT, 128), bf16), pltpu.VMEM((3, HEADS, 128), f32),
            pltpu.SemaphoreType.DMA((HALF,)),
        ], flops // 8,
    )(core, near(own_state), near(got), near(totals))
    collected = lax.all_to_all(block_state, everyone, 0, 0, tiled=True)
    their_first = lax.ppermute(late_own, "core", swap)
    own_first = lax.ppermute(late_theirs, "core", swap)
    other_decay = lax.ppermute(decay, "core", swap)

    block = pl.BlockSpec((2, 1, ROWS, 2 * DV), lambda i, c: (0, i, 0, 0))
    within, reach = call(
        within_kernel, HALF,
        [heads(DK), heads(DK), heads(DV), heads(DV),
         theirs(DK), theirs(DK), theirs(DV), theirs(DV), here, here, decays, decays],
        [block, pl.BlockSpec((ROWS, HEADS), lambda i, c: (0, 0))],
        [pltpu.HBM((2, HALF, ROWS, 2 * DV), f32), pltpu.HBM((ROWS, HEADS), f32)],
        [table, pltpu.VMEM((HEADS, ROWS), f32), table], 4 * flops,
    )(core, far(queries), key_far, value_far, far(gate_input), far(queries), key_far, value_far,
      far(gate_input), near(own_first), near(their_first), decay_far, other_decay)

    starts = pl.pallas_call(
        prefix_kernel,
        out_shape=slices,
        in_specs=[here],
        out_specs=here,
        compiler_params=pltpu.CompilerParams(vmem_limit_bytes=LIMIT * MIB),
        cost_estimate=pl.CostEstimate(flops=10**10, transcendentals=0, bytes_accessed=0),
        name="prefix",
    )(near(collected))
    start = lax.all_to_all(starts, everyone, 0, 0, tiled=True)
    their_start = lax.ppermute(start, "core", swap)

    specs = [here, pl.BlockSpec((ROWS, HEADS), lambda i, c: (0, 0)), here, here]
    result = pltpu.HBM((ROWS, HEADS * DV), bf16)
    done = call(partial(finish_kernel, 0), steps, specs, wide(DV), result, [], flops)(
        core, near(start), far(reach), near(queries), near(within)
    )
    return call(
        partial(finish_kernel, 1), steps, specs + [away], wide(DV), result, [], flops, {5: 0},
    )(other, near(their_start), far(reach), near(queries), near(within), done)


def solution(mesh):
    mesh = Mesh(mesh.devices.reshape(4, 16, 2), ("seq", "chip", "core"))
    spec = P(("seq", "chip", "core"), None)

    return jax.shard_map(shards, mesh=mesh, in_specs=(spec,) * 5, out_specs=spec, check_vma=False)
```

```python
from functools import partial

import jax
import jax.numpy as jnp
from jax import lax
from jax.experimental import pallas as pl
from jax.experimental.pallas import tpu as pltpu
from jax.sharding import Mesh, PartitionSpec as P


HEADS = 16
DK = 256
DV = 512
ROWS = 256
HALF = HEADS // 2
CHIPS = 64
SLICES = CHIPS // HALF
PIECE = DK // SLICES
TILES = DV // 128
SLICE = PIECE * TILES
SENT = SLICE + 8
PER_STEP = 4
MIB = 2**20
LIMIT = 20

f32 = jnp.float32
bf16 = jnp.bfloat16


def triangle():
    rows = lax.broadcasted_iota(jnp.int32, (ROWS, ROWS), 0)
    cols = lax.broadcasted_iota(jnp.int32, (ROWS, ROWS), 1)
    return rows >= cols


def running_of(decay):
    ones = triangle().astype(f32).astype(bf16)
    return lax.dot_general(ones, decay, (((1,), (1,)), ((), ())), preferred_element_type=f32)


def running_rows(decay):
    ones = triangle().astype(f32).astype(bf16)
    return lax.dot_general(decay, ones, (((1,), (1,)), ((), ())), preferred_element_type=f32)


def column(table, head):
    lanes = lax.broadcasted_iota(jnp.int32, table.shape, 1)
    return jnp.sum(jnp.where(lanes == head, table, 0.0), axis=1, keepdims=True)


def put_slices(ref, at, state):
    for o in range(SLICES):
        for t in range(TILES):
            ref[at * SLICES + o, t * PIECE : (t + 1) * PIECE, :] = state[
                o * PIECE : (o + 1) * PIECE, t * 128 : (t + 1) * 128
            ]


def get_slices(ref, at):
    cols = [
        ref[pl.ds(at * SLICES, SLICES), t * PIECE : (t + 1) * PIECE, :].reshape(DK, 128)
        for t in range(TILES)
    ]
    return jnp.concatenate(cols, axis=1)


def start_all(copies):
    for copy in copies:
        copy.start()
    return copies


def states_into(refs, group, step, key_ref, value_ref, fade_ref):
    for n in range(PER_STEP):
        at = step * PER_STEP + n
        fade = column(fade_ref[...], group * HALF + at)
        faded = (key_ref[:, n * DK : (n + 1) * DK].astype(f32) * fade).astype(bf16)
        state = lax.dot_general(
            faded, value_ref[:, n * DV : (n + 1) * DV], (((0,), (0,)), ((), ())),
            preferred_element_type=f32,
        ).astype(bf16)
        for ref, place in zip(refs, (at, n)):
            put_slices(ref, place, state)


def fades_of(decay):
    run = running_of(decay)
    return jnp.exp(run[ROWS - 1 : ROWS, :] - run)


def totals_of(decay):
    ones = jnp.ones((128, ROWS), f32).astype(bf16)
    return lax.dot_general(decay, ones, (((1,), (1,)), ((), ())), preferred_element_type=f32)


def thirds_of(value):
    high = value.astype(bf16).astype(f32)
    rest = value - high
    middle = rest.astype(bf16).astype(f32)
    return high, middle, rest - middle


def theirs_kernel(group_ref, key_ref, value_ref, decay_ref, out_ref, fade_ref):
    step = pl.program_id(0)

    @pl.when(step == 0)
    def _():
        fade_ref[...] = fades_of(decay_ref[...])
        for k, third in enumerate(thirds_of(totals_of(decay_ref[...]))):
            out_ref[CHIPS, k * HEADS : (k + 1) * HEADS, :] = third.astype(bf16)

    states_into((out_ref,), group_ref[0], step, key_ref, value_ref, fade_ref)


def own_kernel(
    group_ref, key_ref, value_ref, decay_ref, theirs_ref,
    out_ref, total_ref, own_copy_ref, theirs_copy_ref, fade_ref,
):
    step = pl.program_id(0)

    @pl.when(step == 0)
    def _():
        fade_ref[...] = fades_of(decay_ref[...])
        total_ref[...] = totals_of(decay_ref[...])

    size = PER_STEP * SLICES
    theirs_copy_ref[...] = theirs_ref[pl.ds(step * size, size)]
    states_into((out_ref, own_copy_ref), group_ref[0], step, key_ref, value_ref, fade_ref)


def combine_kernel(core_ref, own_ref, got_ref, total_ref, out_ref, buf_ref, rate_ref, sems):
    is_first = core_ref[0] == 0
    total = total_ref[...]
    thirds = [got_ref[CHIPS, k * HEADS : (k + 1) * HEADS, :].astype(f32) for k in range(3)]
    other = thirds[0] + thirds[1] + thirds[2]
    rate_ref[0] = jnp.exp(jnp.where(is_first, other, 0.0))
    rate_ref[1] = jnp.exp(jnp.where(is_first, 0.0, total))
    rate_ref[2] = jnp.exp(total + other)
    rows = lax.broadcasted_iota(jnp.int32, (8, 128), 0)
    copies = []
    for n in range(HALF):
        head = pl.ds(core_ref[0] * HALF + n, 1)
        own_rate = rate_ref[0, head, :]
        got_rate = rate_ref[1, head, :]
        high, middle, low = thirds_of(rate_ref[2, head, :])
        parts = jnp.where(rows == 0, high, jnp.where(rows == 1, middle, low))
        parts = parts.astype(bf16)
        for o in range(n * SLICES, (n + 1) * SLICES):
            both = own_ref[o].astype(f32) * own_rate + got_ref[o].astype(f32) * got_rate
            buf_ref[o, :SLICE, :] = both.astype(bf16)
            buf_ref[o, SLICE:SENT, :] = parts
        block = pl.ds(n * SLICES, SLICES)
        copies.extend(start_all((
            pltpu.make_async_copy(buf_ref.at[block], out_ref.at[block], sems.at[n]),
        )))
    for copy in copies:
        copy.wait()


def within_kernel(core_ref, *refs):
    own, theirs, (got_ref, first_ref, decay_ref, other_ref) = refs[0:4], refs[4:8], refs[8:12]
    out_ref, reach_out, run_ref, rows_ref, reach_ref = refs[12:]
    step = pl.program_id(0)
    core = core_ref[0]

    @pl.when(step == 0)
    def _():
        run = running_of(decay_ref[...])
        run_ref[...] = run
        rows_ref[...] = running_rows(decay_ref[...])
        other = running_of(other_ref[...])[ROWS - 1 : ROWS, :]
        reach = jnp.exp(run + jnp.where(core == 0, 0.0, other))
        for h in range(HEADS):
            reach_out[h] = jnp.broadcast_to(reach[:, h : h + 1], (ROWS, 128))
        reach_ref[...] = jnp.where(core == 0, 0.0, jnp.exp(run))

    for side, (group, ins, state_ref) in enumerate((
        (core, own, got_ref), (1 - core, theirs, first_ref),
    )):
        query_ref, key_ref, value_ref, gate_ref = ins
        head = group * HALF + step
        query = query_ref[...]
        scores = lax.dot_general(
            query, key_ref[...], (((1,), (1,)), ((), ())), preferred_element_type=f32
        )
        spread = column(run_ref[...], head) - rows_ref[pl.ds(head, 1), :]
        factor = jnp.exp(jnp.where(triangle(), spread, -jnp.inf))
        weights = (scores * factor).astype(bf16)
        local = jnp.dot(weights, value_ref[...], preferred_element_type=f32)
        before = jnp.dot(query, get_slices(state_ref, step), preferred_element_type=f32)
        inner = local + before * column(reach_ref[...], head)
        out_ref[side, 0, :, :DV] = inner
        gate = 0.5 * gate_ref[...].astype(f32)
        out_ref[side, 0, :, DV:] = gate + gate * jnp.tanh(gate)


def prefix_kernel(in_ref, out_ref):
    state = jnp.zeros((SLICE, 128), f32)
    for b in range(CHIPS):
        parts = in_ref[b, SLICE:SENT, :].astype(f32)
        damping = parts[0:1] + parts[1:2] + parts[2:3]
        out_ref[b] = state.astype(bf16)
        state = damping * state + in_ref[b, :SLICE, :].astype(f32)


def finish_kernel(side, group_ref, start_ref, reach_ref, query_ref, ready_ref, *rest):
    out_ref, buf_ref, sems = rest[-3:]
    copies = []
    for n in range(HALF):
        head = group_ref[0] * HALF + n
        query = query_ref[:, pl.ds(pl.multiple_of(head * DK, DK), DK)]
        across = jnp.dot(query, get_slices(start_ref, n), preferred_element_type=f32)
        reach = jnp.concatenate([reach_ref[head]] * TILES, axis=1)
        retained = ready_ref[side, n, :, :DV] + across * reach
        average = jnp.mean(retained, axis=1, keepdims=True)
        centered = retained - average
        variance = jnp.mean(centered * centered, axis=1, keepdims=True)
        normed = centered * lax.rsqrt(variance + 1e-06)
        buf_ref[:, n * DV : (n + 1) * DV] = (ready_ref[side, n, :, DV:] * normed).astype(bf16)
        place = pl.ds(pl.multiple_of(head * DV, DV), DV)
        copies.extend(start_all((
            pltpu.make_async_copy(
                buf_ref.at[:, pl.ds(n * DV, DV)], out_ref.at[:, place], sems.at[n]
            ),
        )))
    for copy in copies:
        copy.wait()


def call(kernel, grid, in_specs, out_specs, out_shape, scratch, flops, aliases=None):
    return pl.pallas_call(
        kernel,
        out_shape=out_shape,
        grid_spec=pltpu.PrefetchScalarGridSpec(
            num_scalar_prefetch=1,
            grid=(grid,),
            in_specs=in_specs,
            out_specs=out_specs,
            scratch_shapes=scratch,
        ),
        compiler_params=pltpu.CompilerParams(
            dimension_semantics=("arbitrary",), vmem_limit_bytes=LIMIT * MIB
        ),
        cost_estimate=pl.CostEstimate(flops=flops, transcendentals=0, bytes_accessed=0),
        input_output_aliases=aliases or {},
    )


def far(value):
    return pltpu.with_memory_space_constraint(value, pltpu.HBM)


def near(value):
    return pltpu.with_memory_space_constraint(value, pltpu.VMEM)


def shards(queries, key_vectors, values, decay_log, gate_input):
    core = lax.axis_index("core").astype(jnp.int32).reshape(1)
    other = 1 - core
    swap = [(0, 1), (1, 0)]
    everyone = ("seq", "chip")
    decay = decay_log.T

    steps = HALF // PER_STEP
    here = pl.BlockSpec(memory_space=pltpu.VMEM)
    decays = pl.BlockSpec((HEADS, ROWS), lambda i, c: (0, 0))
    heads = lambda width: pl.BlockSpec((ROWS, width), lambda i, c: (0, c[0] * HALF + i))
    theirs = lambda width: pl.BlockSpec((ROWS, width), lambda i, c: (0, (1 - c[0]) * HALF + i))
    table = pltpu.VMEM((ROWS, HEADS), f32)
    flops = 2 * HALF * ROWS * DK * DV
    slices = pltpu.VMEM((CHIPS, SLICE, 128), bf16)

    away = pl.BlockSpec(memory_space=pl.ANY)
    key_far, value_far, decay_far = far(key_vectors), far(values), far(decay)
    stored = pltpu.HBM((CHIPS, SLICE, 128), bf16)
    wide = lambda width: pl.BlockSpec(
        (ROWS, width * PER_STEP), lambda i, c: (0, c[0] * steps + i)
    )
    pieces = pl.BlockSpec((SLICES * PER_STEP, SLICE, 128), lambda i, c: (i, 0, 0))
    theirs_state = call(
        theirs_kernel, steps, [wide(DK), wide(DV), decays], here,
        pltpu.VMEM((CHIPS + 1, SLICE, 128), bf16), [table], flops
    )(other, key_far, value_far, decay_far)
    got = lax.ppermute(theirs_state, "core", swap)
    own_state, totals, late_own, late_theirs = call(
        own_kernel, steps, [wide(DK), wide(DV), decays, here],
        [here, here, pieces, pieces],
        [slices, pltpu.VMEM((HEADS, 128), f32), stored, stored],
        [table], flops,
    )(core, key_far, value_far, decay_far, near(theirs_state))
    block_state = call(
        combine_kernel, 1, [here, here, here], away,
        pltpu.HBM((CHIPS, SENT, 128), bf16),
        [
            pltpu.VMEM((CHIPS, SENT, 128), bf16), pltpu.VMEM((3, HEADS, 128), f32),
            pltpu.SemaphoreType.DMA((HALF,)),
        ], flops // 8,
    )(core, near(own_state), near(got), near(totals))
    collected = lax.all_to_all(block_state, everyone, 0, 0, tiled=True)
    their_first = lax.ppermute(late_own, "core", swap)
    own_first = lax.ppermute(late_theirs, "core", swap)
    other_decay = lax.ppermute(decay, "core", swap)

    block = pl.BlockSpec((2, 1, ROWS, 2 * DV), lambda i, c: (0, i, 0, 0))
    within, reach = call(
        within_kernel, HALF,
        [heads(DK), heads(DK), heads(DV), heads(DV),
         theirs(DK), theirs(DK), theirs(DV), theirs(DV), here, here, decays, decays],
        [block, pl.BlockSpec((HEADS, ROWS, 128), lambda i, c: (0, 0, 0))],
        [pltpu.HBM((2, HALF, ROWS, 2 * DV), f32), pltpu.HBM((HEADS, ROWS, 128), f32)],
        [table, pltpu.VMEM((HEADS, ROWS), f32), table], 4 * flops,
    )(core, far(queries), key_far, value_far, far(gate_input), far(queries), key_far, value_far,
      far(gate_input), near(own_first), near(their_first), decay_far, other_decay)

    starts = pl.pallas_call(
        prefix_kernel,
        out_shape=slices,
        in_specs=[here],
        out_specs=here,
        compiler_params=pltpu.CompilerParams(vmem_limit_bytes=LIMIT * MIB),
        cost_estimate=pl.CostEstimate(flops=10**10, transcendentals=0, bytes_accessed=0),
        name="prefix",
    )(near(collected))
    start = lax.all_to_all(starts, everyone, 0, 0, tiled=True)
    their_start = lax.ppermute(start, "core", swap)

    specs = [here] * 4
    result = pltpu.HBM((ROWS, HEADS * DV), bf16)
    scratch = [pltpu.VMEM((ROWS, HALF * DV), bf16), pltpu.SemaphoreType.DMA((HALF,))]
    ready = [near(reach), near(queries), near(within)]
    done = call(partial(finish_kernel, 0), 1, specs, away, result, scratch, flops)(
        core, near(start), *ready
    )
    return call(
        partial(finish_kernel, 1), 1, specs + [away], away, result, scratch, flops,
        {5: 0},
    )(other, near(their_start), *ready, done)


def solution(mesh):
    mesh = Mesh(mesh.devices.reshape(4, 16, 2), ("seq", "chip", "core"))
    spec = P(("seq", "chip", "core"), None)

    return jax.shard_map(shards, mesh=mesh, in_specs=(spec,) * 5, out_specs=spec, check_vma=False)
```

```python
from functools import partial

import jax
import jax.numpy as jnp
from jax import lax
from jax.experimental import pallas as pl
from jax.experimental.pallas import tpu as pltpu
from jax.sharding import Mesh, PartitionSpec as P


HEADS = 16
DK = 256
DV = 512
ROWS = 256
HALF = HEADS // 2
CHIPS = 64
SLICES = CHIPS // HALF
PIECE = DK // SLICES
TILES = DV // 128
SLICE = PIECE * TILES
LINE = 4
PER_STEP = 4
MIB = 2**20
LIMIT = 20

f32 = jnp.float32
bf16 = jnp.bfloat16


def triangle():
    rows = lax.broadcasted_iota(jnp.int32, (ROWS, ROWS), 0)
    cols = lax.broadcasted_iota(jnp.int32, (ROWS, ROWS), 1)
    return rows >= cols


def running_of(decay):
    ones = triangle().astype(f32).astype(bf16)
    return lax.dot_general(ones, decay, (((1,), (1,)), ((), ())), preferred_element_type=f32)


def running_rows(decay):
    ones = triangle().astype(f32).astype(bf16)
    return lax.dot_general(decay, ones, (((1,), (1,)), ((), ())), preferred_element_type=f32)


def column(table, head):
    lanes = lax.broadcasted_iota(jnp.int32, table.shape, 1)
    return jnp.sum(jnp.where(lanes == head, table, 0.0), axis=1, keepdims=True)


def put_slices(ref, at, state):
    for o in range(SLICES):
        for t in range(TILES):
            ref[at * SLICES + o, t * PIECE : (t + 1) * PIECE, :] = state[
                o * PIECE : (o + 1) * PIECE, t * 128 : (t + 1) * 128
            ]


def get_slices(ref, at):
    cols = [
        ref[pl.ds(at * SLICES, SLICES), t * PIECE : (t + 1) * PIECE, :].reshape(DK, 128)
        for t in range(TILES)
    ]
    return jnp.concatenate(cols, axis=1)


def start_all(copies):
    for copy in copies:
        copy.start()
    return copies


def states_into(refs, group, step, key_ref, value_ref, fade_ref):
    for n in range(PER_STEP):
        at = step * PER_STEP + n
        fade = column(fade_ref[...], group * HALF + at)
        faded = (key_ref[:, n * DK : (n + 1) * DK].astype(f32) * fade).astype(bf16)
        state = lax.dot_general(
            faded, value_ref[:, n * DV : (n + 1) * DV], (((0,), (0,)), ((), ())),
            preferred_element_type=f32,
        ).astype(bf16)
        for ref, place in zip(refs, (at, n)):
            put_slices(ref, place, state)


def fades_of(decay):
    run = running_of(decay)
    return jnp.exp(run[ROWS - 1 : ROWS, :] - run)


def totals_of(decay):
    ones = jnp.ones((128, ROWS), f32).astype(bf16)
    return lax.dot_general(decay, ones, (((1,), (1,)), ((), ())), preferred_element_type=f32)


def thirds_of(value):
    high = value.astype(bf16).astype(f32)
    rest = value - high
    middle = rest.astype(bf16).astype(f32)
    return high, middle, rest - middle


def theirs_kernel(group_ref, key_ref, value_ref, decay_ref, out_ref, fade_ref):
    step = pl.program_id(0)

    @pl.when(step == 0)
    def _():
        fade_ref[...] = fades_of(decay_ref[...])
        for k, third in enumerate(thirds_of(totals_of(decay_ref[...]))):
            out_ref[CHIPS, k * HEADS : (k + 1) * HEADS, :] = third.astype(bf16)

    states_into((out_ref,), group_ref[0], step, key_ref, value_ref, fade_ref)


def own_kernel(
    group_ref, key_ref, value_ref, decay_ref, theirs_ref,
    out_ref, total_ref, own_copy_ref, theirs_copy_ref, fade_ref,
):
    step = pl.program_id(0)

    @pl.when(step == 0)
    def _():
        fade_ref[...] = fades_of(decay_ref[...])
        total_ref[...] = totals_of(decay_ref[...])

    size = PER_STEP * SLICES
    theirs_copy_ref[...] = theirs_ref[pl.ds(step * size, size)]
    states_into((out_ref, own_copy_ref), group_ref[0], step, key_ref, value_ref, fade_ref)


def combine_kernel(core_ref, own_ref, got_ref, total_ref, out_ref, damp_ref, buf_ref, rate_ref, sems):
    is_first = core_ref[0] == 0
    total = total_ref[...]
    thirds = [got_ref[CHIPS, k * HEADS : (k + 1) * HEADS, :].astype(f32) for k in range(3)]
    other = thirds[0] + thirds[1] + thirds[2]
    rate_ref[0] = jnp.exp(jnp.where(is_first, other, 0.0))
    rate_ref[1] = jnp.exp(jnp.where(is_first, 0.0, total))
    rate_ref[2] = jnp.exp(total + other)
    damp_ref[...] = rate_ref[2, pl.ds(pl.multiple_of(core_ref[0] * HALF, HALF), HALF), :]
    copies = []
    for n in range(HALF):
        head = pl.ds(core_ref[0] * HALF + n, 1)
        own_rate = rate_ref[0, head, :]
        got_rate = rate_ref[1, head, :]
        for o in range(n * SLICES, (n + 1) * SLICES):
            both = own_ref[o].astype(f32) * own_rate + got_ref[o].astype(f32) * got_rate
            buf_ref[o] = both.astype(bf16)
        block = pl.ds(n * SLICES, SLICES)
        copies.extend(start_all((
            pltpu.make_async_copy(buf_ref.at[block], out_ref.at[block], sems.at[n]),
        )))
    for copy in copies:
        copy.wait()


def within_kernel(core_ref, *refs):
    own, theirs, (got_ref, first_ref, decay_ref, other_ref) = refs[0:3], refs[3:6], refs[6:10]
    out_ref, reach_out, run_ref, rows_ref, reach_ref = refs[10:]
    step = pl.program_id(0)
    core = core_ref[0]

    @pl.when(step == 0)
    def _():
        run = running_of(decay_ref[...])
        run_ref[...] = run
        rows_ref[...] = running_rows(decay_ref[...])
        other = running_of(other_ref[...])[ROWS - 1 : ROWS, :]
        reach = jnp.exp(run + jnp.where(core == 0, 0.0, other))
        for h in range(HEADS):
            reach_out[h] = jnp.broadcast_to(reach[:, h : h + 1], (ROWS, 128))
        reach_ref[...] = jnp.where(core == 0, 0.0, jnp.exp(run))

    for side, (group, ins, state_ref) in enumerate((
        (core, own, got_ref), (1 - core, theirs, first_ref),
    )):
        query_ref, key_ref, value_ref = ins
        head = group * HALF + step
        query = query_ref[...]
        scores = lax.dot_general(
            query, key_ref[...], (((1,), (1,)), ((), ())), preferred_element_type=f32
        )
        spread = column(run_ref[...], head) - rows_ref[pl.ds(head, 1), :]
        factor = jnp.exp(jnp.where(triangle(), spread, -jnp.inf))
        weights = (scores * factor).astype(bf16)
        local = jnp.dot(weights, value_ref[...], preferred_element_type=f32)
        before = jnp.dot(query, get_slices(state_ref, step), preferred_element_type=f32)
        inner = local + before * column(reach_ref[...], head)
        out_ref[side, 0] = inner


def prefix_kernel(place_ref, in_ref, *refs):
    ins, out_ref, damp_ref = refs[:LINE], refs[LINE], refs[LINE + 1]
    for d in range(LINE):
        damp_ref[d * LINE * LINE : (d + 1) * LINE * LINE] = ins[d][...]
    x, y, z = place_ref[0], place_ref[1], place_ref[2]
    head = pl.ds((x * LINE * LINE + y * LINE + z) // SLICES, 1)
    state = jnp.zeros((SLICE, 128), f32)
    for b in range(CHIPS):
        apart = [(here + LINE - b // far % LINE) % LINE for here, far in ((x, 16), (y, 4), (z, 1))]
        damping = damp_ref[apart[0] * LINE * LINE + apart[1] * LINE + apart[2], head, :]
        out_ref[b] = state.astype(bf16)
        state = damping * state + in_ref[b].astype(f32)


def finish_kernel(side, group_ref, start_ref, reach_ref, query_ref, ready_ref, gate_ref, *rest):
    out_ref, buf_ref, sems = rest[-3:]
    copies = []
    for n in range(HALF):
        head = group_ref[0] * HALF + n
        query = query_ref[:, pl.ds(pl.multiple_of(head * DK, DK), DK)]
        across = jnp.dot(query, get_slices(start_ref, n), preferred_element_type=f32)
        reach = jnp.concatenate([reach_ref[head]] * TILES, axis=1)
        retained = ready_ref[side, n] + across * reach
        average = jnp.mean(retained, axis=1, keepdims=True)
        centered = retained - average
        variance = jnp.mean(centered * centered, axis=1, keepdims=True)
        normed = centered * lax.rsqrt(variance + 1e-06)
        place = pl.ds(pl.multiple_of(head * DV, DV), DV)
        gate = 0.5 * gate_ref[:, place].astype(f32)
        gated = (gate + gate * jnp.tanh(gate)) * normed
        buf_ref[:, n * DV : (n + 1) * DV] = gated.astype(bf16)
        copies.extend(start_all((
            pltpu.make_async_copy(
                buf_ref.at[:, pl.ds(n * DV, DV)], out_ref.at[:, place], sems.at[n]
            ),
        )))
    for copy in copies:
        copy.wait()


def call(kernel, grid, in_specs, out_specs, out_shape, scratch, flops, aliases=None):
    return pl.pallas_call(
        kernel,
        out_shape=out_shape,
        grid_spec=pltpu.PrefetchScalarGridSpec(
            num_scalar_prefetch=1,
            grid=(grid,),
            in_specs=in_specs,
            out_specs=out_specs,
            scratch_shapes=scratch,
        ),
        compiler_params=pltpu.CompilerParams(
            dimension_semantics=("arbitrary",), vmem_limit_bytes=LIMIT * MIB
        ),
        cost_estimate=pl.CostEstimate(flops=flops, transcendentals=0, bytes_accessed=0),
        input_output_aliases=aliases or {},
    )


def far(value):
    return pltpu.with_memory_space_constraint(value, pltpu.HBM)


def near(value):
    return pltpu.with_memory_space_constraint(value, pltpu.VMEM)


def shifted(value, axis):
    shifts = [[(i, (i + d) % LINE) for i in range(LINE)] for d in range(1, LINE)]
    return [value] + [lax.ppermute(value, axis, pairs) for pairs in shifts]


def join_kernel(*refs):
    size = refs[0].shape[0]
    for d, ref in enumerate(refs[:LINE]):
        refs[LINE][d * size : (d + 1) * size] = ref[...]


def joined(parts):
    here = pl.BlockSpec(memory_space=pltpu.VMEM)
    return pl.pallas_call(
        join_kernel,
        out_shape=pltpu.VMEM((LINE * parts[0].shape[0], *parts[0].shape[1:]), f32),
        in_specs=[here] * LINE,
        out_specs=here,
        compiler_params=pltpu.CompilerParams(vmem_limit_bytes=LIMIT * MIB),
        name="join",
    )(*map(near, parts))


def shards(queries, key_vectors, values, decay_log, gate_input):
    core = lax.axis_index("core").astype(jnp.int32).reshape(1)
    other = 1 - core
    swap = [(0, 1), (1, 0)]
    everyone = ("x", "y", "z")
    decay = decay_log.T

    steps = HALF // PER_STEP
    here = pl.BlockSpec(memory_space=pltpu.VMEM)
    decays = pl.BlockSpec((HEADS, ROWS), lambda i, c: (0, 0))
    heads = lambda width: pl.BlockSpec((ROWS, width), lambda i, c: (0, c[0] * HALF + i))
    theirs = lambda width: pl.BlockSpec((ROWS, width), lambda i, c: (0, (1 - c[0]) * HALF + i))
    table = pltpu.VMEM((ROWS, HEADS), f32)
    flops = 2 * HALF * ROWS * DK * DV
    slices = pltpu.VMEM((CHIPS, SLICE, 128), bf16)

    away = pl.BlockSpec(memory_space=pl.ANY)
    key_far, value_far, decay_far = far(key_vectors), far(values), far(decay)
    stored = pltpu.HBM((CHIPS, SLICE, 128), bf16)
    wide = lambda width: pl.BlockSpec(
        (ROWS, width * PER_STEP), lambda i, c: (0, c[0] * steps + i)
    )
    pieces = pl.BlockSpec((SLICES * PER_STEP, SLICE, 128), lambda i, c: (i, 0, 0))
    theirs_state = call(
        theirs_kernel, steps, [wide(DK), wide(DV), decays], here,
        pltpu.VMEM((CHIPS + 1, SLICE, 128), bf16), [table], flops
    )(other, key_far, value_far, decay_far)
    got = lax.ppermute(theirs_state, "core", swap)
    own_state, totals, late_own, late_theirs = call(
        own_kernel, steps, [wide(DK), wide(DV), decays, here],
        [here, here, pieces, pieces],
        [slices, pltpu.VMEM((HEADS, 128), f32), stored, stored],
        [table], flops,
    )(core, key_far, value_far, decay_far, near(theirs_state))
    block_state, damping = call(
        combine_kernel, 1, [here, here, here], [away, here],
        [pltpu.HBM((CHIPS, SLICE, 128), bf16), pltpu.VMEM((HALF, 128), f32)],
        [
            pltpu.VMEM((CHIPS, SLICE, 128), bf16), pltpu.VMEM((3, HEADS, 128), f32),
            pltpu.SemaphoreType.DMA((HALF,)),
        ], flops // 8,
    )(core, near(own_state), near(got), near(totals))
    collected = lax.all_to_all(block_state, everyone, 0, 0, tiled=True)
    along_line = joined(shifted(damping[None], "z"))
    along_plane = joined(shifted(along_line, "y"))
    dampings = shifted(along_plane, "x")
    their_first = lax.ppermute(late_own, "core", swap)
    own_first = lax.ppermute(late_theirs, "core", swap)
    other_decay = lax.ppermute(decay, "core", swap)

    block = pl.BlockSpec((2, 1, ROWS, DV), lambda i, c: (0, i, 0, 0))
    within, reach = call(
        within_kernel, HALF,
        [heads(DK), heads(DK), heads(DV), theirs(DK), theirs(DK), theirs(DV), here, here, decays, decays],
        [block, pl.BlockSpec((HEADS, ROWS, 128), lambda i, c: (0, 0, 0))],
        [pltpu.HBM((2, HALF, ROWS, DV), f32), pltpu.HBM((HEADS, ROWS, 128), f32)],
        [table, pltpu.VMEM((HEADS, ROWS), f32), table], 4 * flops,
    )(core, far(queries), key_far, value_far, far(queries), key_far, value_far,
      near(own_first), near(their_first), decay_far, other_decay)

    place = jnp.stack([lax.axis_index(a) for a in ("x", "y", "z")]).astype(jnp.int32)
    starts = call(
        prefix_kernel, 1, [here] * (1 + LINE), here, slices,
        [pltpu.VMEM((CHIPS, HALF, 128), f32)], 10**10,
    )(place, near(collected), *map(near, dampings))
    start = lax.all_to_all(starts, everyone, 0, 0, tiled=True)
    their_start = lax.ppermute(start, "core", swap)

    specs = [here] * 5
    result = pltpu.HBM((ROWS, HEADS * DV), bf16)
    scratch = [pltpu.VMEM((ROWS, HALF * DV), bf16), pltpu.SemaphoreType.DMA((HALF,))]
    ready = [near(reach), near(queries), near(within), near(gate_input)]
    done = call(partial(finish_kernel, 0), 1, specs, away, result, scratch, flops)(
        core, near(start), *ready
    )
    return call(
        partial(finish_kernel, 1), 1, specs + [away], away, result, scratch, flops,
        {6: 0},
    )(other, near(their_start), *ready, done)


def solution(mesh):
    mesh = Mesh(mesh.devices.reshape(4, 4, 4, 2), ("x", "y", "z", "core"))
    spec = P(("x", "y", "z", "core"), None)

    return jax.shard_map(shards, mesh=mesh, in_specs=(spec,) * 5, out_specs=spec, check_vma=False)
```

```python
from functools import partial

import jax
import jax.numpy as jnp
from jax import lax
from jax.experimental import pallas as pl
from jax.experimental.pallas import tpu as pltpu
from jax.sharding import Mesh, PartitionSpec as P


HEADS = 16
DK = 256
DV = 512
ROWS = 256
HALF = HEADS // 2
CHIPS = 64
SLICES = CHIPS // HALF
PIECE = DK // SLICES
TILES = DV // 128
SLICE = PIECE * TILES
SENT = SLICE + 8
PER_STEP = 4
MIB = 2**20
LIMIT = 20

f32 = jnp.float32
bf16 = jnp.bfloat16


def triangle():
    rows = lax.broadcasted_iota(jnp.int32, (ROWS, ROWS), 0)
    cols = lax.broadcasted_iota(jnp.int32, (ROWS, ROWS), 1)
    return rows >= cols


def running_of(decay):
    ones = triangle().astype(f32).astype(bf16)
    return lax.dot_general(ones, decay, (((1,), (1,)), ((), ())), preferred_element_type=f32)


def running_rows(decay):
    ones = triangle().astype(f32).astype(bf16)
    return lax.dot_general(decay, ones, (((1,), (1,)), ((), ())), preferred_element_type=f32)


def column(table, head):
    lanes = lax.broadcasted_iota(jnp.int32, table.shape, 1)
    return jnp.sum(jnp.where(lanes == head, table, 0.0), axis=1, keepdims=True)


def put_slices(ref, at, state):
    for o in range(SLICES):
        for t in range(TILES):
            ref[at * SLICES + o, t * PIECE : (t + 1) * PIECE, :] = state[
                o * PIECE : (o + 1) * PIECE, t * 128 : (t + 1) * 128
            ]


def get_slices(ref, at):
    cols = [
        ref[pl.ds(at * SLICES, SLICES), t * PIECE : (t + 1) * PIECE, :].reshape(DK, 128)
        for t in range(TILES)
    ]
    return jnp.concatenate(cols, axis=1)


def start_all(copies):
    for copy in copies:
        copy.start()
    return copies


def states_into(refs, step, key_ref, value_ref, fade_ref):
    for n in range(PER_STEP):
        at = step * PER_STEP + n
        fade = jnp.concatenate([fade_ref[at]] * (DK // 128), axis=1)
        faded = (key_ref[:, n * DK : (n + 1) * DK].astype(f32) * fade).astype(bf16)
        state = lax.dot_general(
            faded, value_ref[:, n * DV : (n + 1) * DV], (((0,), (0,)), ((), ())),
            preferred_element_type=f32,
        ).astype(bf16)
        for ref, place in zip(refs, (at, n)):
            put_slices(ref, place, state)


def put_fades(ref, decay, group):
    run = running_of(decay)
    fades = jnp.exp(run[ROWS - 1 : ROWS, :] - run)
    for n in range(HALF):
        ref[n] = jnp.broadcast_to(column(fades, group * HALF + n), (ROWS, 128))


def totals_of(decay):
    ones = jnp.ones((128, ROWS), f32).astype(bf16)
    return lax.dot_general(decay, ones, (((1,), (1,)), ((), ())), preferred_element_type=f32)


def thirds_of(value):
    high = value.astype(bf16).astype(f32)
    rest = value - high
    middle = rest.astype(bf16).astype(f32)
    return high, middle, rest - middle


def theirs_kernel(group_ref, key_ref, value_ref, decay_ref, out_ref, fade_ref):
    step = pl.program_id(0)

    @pl.when(step == 0)
    def _():
        put_fades(fade_ref, decay_ref[...], group_ref[0])
        for k, third in enumerate(thirds_of(totals_of(decay_ref[...]))):
            out_ref[CHIPS, k * HEADS : (k + 1) * HEADS, :] = third.astype(bf16)

    states_into((out_ref,), step, key_ref, value_ref, fade_ref)


def own_kernel(
    group_ref, key_ref, value_ref, decay_ref, theirs_ref,
    out_ref, total_ref, own_copy_ref, theirs_copy_ref, fade_ref,
):
    step = pl.program_id(0)

    @pl.when(step == 0)
    def _():
        put_fades(fade_ref, decay_ref[...], group_ref[0])
        total_ref[...] = totals_of(decay_ref[...])

    size = PER_STEP * SLICES
    theirs_copy_ref[...] = theirs_ref[pl.ds(step * size, size)]
    states_into((out_ref, own_copy_ref), step, key_ref, value_ref, fade_ref)


def combine_kernel(core_ref, own_ref, got_ref, total_ref, out_ref, buf_ref, rate_ref, sems):
    is_first = core_ref[0] == 0
    total = total_ref[...]
    thirds = [got_ref[CHIPS, k * HEADS : (k + 1) * HEADS, :].astype(f32) for k in range(3)]
    other = thirds[0] + thirds[1] + thirds[2]
    rate_ref[0] = jnp.exp(jnp.where(is_first, other, 0.0))
    rate_ref[1] = jnp.exp(jnp.where(is_first, 0.0, total))
    rate_ref[2] = jnp.exp(total + other)
    rows = lax.broadcasted_iota(jnp.int32, (8, 128), 0)
    copies = []
    for n in range(HALF):
        head = pl.ds(core_ref[0] * HALF + n, 1)
        own_rate = rate_ref[0, head, :]
        got_rate = rate_ref[1, head, :]
        high, middle, low = thirds_of(rate_ref[2, head, :])
        parts = jnp.where(rows == 0, high, jnp.where(rows == 1, middle, low))
        parts = parts.astype(bf16)
        for o in range(n * SLICES, (n + 1) * SLICES):
            both = own_ref[o].astype(f32) * own_rate + got_ref[o].astype(f32) * got_rate
            buf_ref[o, :SLICE, :] = both.astype(bf16)
            buf_ref[o, SLICE:SENT, :] = parts
        if n % 2 == 0:
            continue
        block = pl.ds((n - 1) * SLICES, 2 * SLICES)
        copies.extend(start_all((
            pltpu.make_async_copy(buf_ref.at[block], out_ref.at[block], sems.at[n]),
        )))
    for copy in copies:
        copy.wait()


def within_kernel(core_ref, *refs):
    own, theirs, (got_ref, first_ref, decay_ref, other_ref) = refs[0:4], refs[4:8], refs[8:12]
    out_ref, reach_out, run_ref, rows_ref, reach_ref = refs[12:]
    step = pl.program_id(0)
    core = core_ref[0]

    @pl.when(step == 0)
    def _():
        run = running_of(decay_ref[...])
        run_ref[...] = run
        rows_ref[...] = running_rows(decay_ref[...])
        other = running_of(other_ref[...])[ROWS - 1 : ROWS, :]
        reach = jnp.exp(run + jnp.where(core == 0, 0.0, other))
        for h in range(HEADS):
            reach_out[h] = jnp.broadcast_to(reach[:, h : h + 1], (ROWS, 128))
        reach_ref[...] = jnp.where(core == 0, 0.0, jnp.exp(run))

    for side, (group, ins, state_ref) in enumerate((
        (core, own, got_ref), (1 - core, theirs, first_ref),
    )):
        query_ref, key_ref, value_ref, gate_ref = ins
        head = group * HALF + step
        query = query_ref[...]
        scores = lax.dot_general(
            query, key_ref[...], (((1,), (1,)), ((), ())), preferred_element_type=f32
        )
        spread = column(run_ref[...], head) - rows_ref[pl.ds(head, 1), :]
        factor = jnp.exp(jnp.where(triangle(), spread, -jnp.inf))
        weights = (scores * factor).astype(bf16)
        local = jnp.dot(weights, value_ref[...], preferred_element_type=f32)
        before = jnp.dot(query, get_slices(state_ref, step), preferred_element_type=f32)
        inner = local + before * column(reach_ref[...], head)
        out_ref[side, 0, :, :DV] = inner
        gate = 0.5 * gate_ref[...].astype(f32)
        out_ref[side, 0, :, DV:] = gate + gate * jnp.tanh(gate)


def prefix_kernel(in_ref, out_ref):
    state = jnp.zeros((SLICE, 128), f32)
    for b in range(CHIPS):
        parts = in_ref[b, SLICE:SENT, :].astype(f32)
        damping = parts[0:1] + parts[1:2] + parts[2:3]
        out_ref[b] = state.astype(bf16)
        state = damping * state + in_ref[b, :SLICE, :].astype(f32)


def finish_kernel(side, group_ref, start_ref, reach_ref, query_ref, ready_ref, *rest):
    out_ref, buf_ref, sems = rest[-3:]
    copies = []
    for n in range(HALF):
        head = group_ref[0] * HALF + n
        query = query_ref[:, pl.ds(pl.multiple_of(head * DK, DK), DK)]
        across = jnp.dot(query, get_slices(start_ref, n), preferred_element_type=f32)
        reach = jnp.concatenate([reach_ref[head]] * TILES, axis=1)
        retained = ready_ref[side, n, :, :DV] + across * reach
        average = jnp.mean(retained, axis=1, keepdims=True)
        centered = retained - average
        variance = jnp.mean(centered * centered, axis=1, keepdims=True)
        normed = centered * lax.rsqrt(variance + 1e-06)
        buf_ref[:, n * DV : (n + 1) * DV] = (ready_ref[side, n, :, DV:] * normed).astype(bf16)
        place = pl.ds(pl.multiple_of(head * DV, DV), DV)
        copies.extend(start_all((
            pltpu.make_async_copy(
                buf_ref.at[:, pl.ds(n * DV, DV)], out_ref.at[:, place], sems.at[n]
            ),
        )))
    for copy in copies:
        copy.wait()


def call(kernel, grid, in_specs, out_specs, out_shape, scratch, flops, aliases=None):
    return pl.pallas_call(
        kernel,
        out_shape=out_shape,
        grid_spec=pltpu.PrefetchScalarGridSpec(
            num_scalar_prefetch=1,
            grid=(grid,),
            in_specs=in_specs,
            out_specs=out_specs,
            scratch_shapes=scratch,
        ),
        compiler_params=pltpu.CompilerParams(
            dimension_semantics=("arbitrary",), vmem_limit_bytes=LIMIT * MIB
        ),
        cost_estimate=pl.CostEstimate(flops=flops, transcendentals=0, bytes_accessed=0),
        input_output_aliases=aliases or {},
    )


def far(value):
    return pltpu.with_memory_space_constraint(value, pltpu.HBM)


def near(value):
    return pltpu.with_memory_space_constraint(value, pltpu.VMEM)


def shards(queries, key_vectors, values, decay_log, gate_input):
    core = lax.axis_index("core").astype(jnp.int32).reshape(1)
    other = 1 - core
    swap = [(0, 1), (1, 0)]
    everyone = ("seq", "chip")
    decay = decay_log.T

    steps = HALF // PER_STEP
    here = pl.BlockSpec(memory_space=pltpu.VMEM)
    decays = pl.BlockSpec((HEADS, ROWS), lambda i, c: (0, 0))
    heads = lambda width: pl.BlockSpec((ROWS, width), lambda i, c: (0, c[0] * HALF + i))
    theirs = lambda width: pl.BlockSpec((ROWS, width), lambda i, c: (0, (1 - c[0]) * HALF + i))
    table = pltpu.VMEM((ROWS, HEADS), f32)
    flops = 2 * HALF * ROWS * DK * DV
    slices = pltpu.VMEM((CHIPS, SLICE, 128), bf16)

    away = pl.BlockSpec(memory_space=pl.ANY)
    fades = pltpu.VMEM((HALF, ROWS, 128), f32)
    key_far, value_far, decay_far = far(key_vectors), far(values), far(decay)
    stored = pltpu.HBM((CHIPS, SLICE, 128), bf16)
    wide = lambda width: pl.BlockSpec(
        (ROWS, width * PER_STEP), lambda i, c: (0, c[0] * steps + i)
    )
    pieces = pl.BlockSpec((SLICES * PER_STEP, SLICE, 128), lambda i, c: (i, 0, 0))
    theirs_state = call(
        theirs_kernel, steps, [wide(DK), wide(DV), decays], here,
        pltpu.VMEM((CHIPS + 1, SLICE, 128), bf16), [fades], flops
    )(other, key_far, value_far, decay_far)
    got = lax.ppermute(theirs_state, "core", swap)
    own_state, totals, late_own, late_theirs = call(
        own_kernel, steps, [wide(DK), wide(DV), decays, here],
        [here, here, pieces, pieces],
        [slices, pltpu.VMEM((HEADS, 128), f32), stored, stored],
        [fades], flops,
    )(core, key_far, value_far, decay_far, near(theirs_state))
    block_state = call(
        combine_kernel, 1, [here, here, here], away,
        pltpu.HBM((CHIPS, SENT, 128), bf16),
        [
            pltpu.VMEM((CHIPS, SENT, 128), bf16), pltpu.VMEM((3, HEADS, 128), f32),
            pltpu.SemaphoreType.DMA((HALF,)),
        ], flops // 8,
    )(core, near(own_state), near(got), near(totals))
    collected = lax.all_to_all(block_state, everyone, 0, 0, tiled=True)
    their_first = lax.ppermute(late_own, "core", swap)
    own_first = lax.ppermute(late_theirs, "core", swap)
    other_decay = lax.ppermute(decay, "core", swap)

    block = pl.BlockSpec((2, 1, ROWS, 2 * DV), lambda i, c: (0, i, 0, 0))
    within, reach = call(
        within_kernel, HALF,
        [heads(DK), heads(DK), heads(DV), heads(DV),
         theirs(DK), theirs(DK), theirs(DV), theirs(DV), here, here, decays, decays],
        [block, pl.BlockSpec((HEADS, ROWS, 128), lambda i, c: (0, 0, 0))],
        [pltpu.HBM((2, HALF, ROWS, 2 * DV), f32), pltpu.HBM((HEADS, ROWS, 128), f32)],
        [table, pltpu.VMEM((HEADS, ROWS), f32), table], 4 * flops,
    )(core, far(queries), key_far, value_far, far(gate_input), far(queries), key_far, value_far,
      far(gate_input), near(own_first), near(their_first), decay_far, other_decay)

    starts = pl.pallas_call(
        prefix_kernel,
        out_shape=slices,
        in_specs=[here],
        out_specs=here,
        compiler_params=pltpu.CompilerParams(vmem_limit_bytes=LIMIT * MIB),
        cost_estimate=pl.CostEstimate(flops=10**10, transcendentals=0, bytes_accessed=0),
        name="prefix",
    )(near(collected))
    start = lax.all_to_all(starts, everyone, 0, 0, tiled=True)
    their_start = lax.ppermute(start, "core", swap)

    specs = [here] * 4
    result = pltpu.HBM((ROWS, HEADS * DV), bf16)
    scratch = [pltpu.VMEM((ROWS, HALF * DV), bf16), pltpu.SemaphoreType.DMA((HALF,))]
    ready = [near(reach), near(queries), near(within)]
    done = call(partial(finish_kernel, 0), 1, specs, away, result, scratch, flops)(
        core, near(start), *ready
    )
    return call(
        partial(finish_kernel, 1), 1, specs + [away], away, result, scratch, flops,
        {5: 0},
    )(other, near(their_start), *ready, done)


def solution(mesh):
    mesh = Mesh(mesh.devices.reshape(4, 16, 2), ("seq", "chip", "core"))
    spec = P(("seq", "chip", "core"), None)

    return jax.shard_map(shards, mesh=mesh, in_specs=(spec,) * 5, out_specs=spec, check_vma=False)
```
